32 devices in a mesh: map: 8 (over z, y), rep: 4 (over x, core).
Axes of the slice: x: 2, y: 2, z: 4, core: 2. Of those that a mesh axis runs over, the one named last changes fastest.
Arguments:
- field_bricks: bfloat16 [16384, 512], P('map'), may hold values from -6 to 6
- owners: int32 [2048, 64], P('map', 'rep'), may hold values from 0 to 7, as said below
- bricks: int32 [2048, 64], P('map', 'rep'), may hold values from 0 to 2047
- corners: int32 [2048, 64], P('map', 'rep'), may hold values from 0 to 342
- fraction: float32 [3, 2048, 64], P(None, 'map', 'rep'), may hold values from 0 to 1
Outputs:
- trajectory_cost: float32 [2048], P('map')
- waypoint_grad: float32 [3, 2048, 64], P(None, 'map', 'rep')
The draws below stay inside these ranges and needn't reach their ends.
Inputs may be any that keep to these rules, and one draw needn't show every extreme that they name: `owners`: among one device's 4096 waypoints at most 2048 have the same owner, and in every draw some owner has exactly 2048 of them.
All inputs are finite; a program needn't handle non-finite values.
Results may differ from the reference program's by a relative error of at most 0.0003.
Values sent between devices are 32-bit elements; how exact they have to be, the bound alone decides.
A program may use at most 64 MiB of HBM per device.

```python
import jax
import jax.numpy as jnp

VOXELS = 512
WAYPOINTS = 64
BRICK_DEV = 2048
TRAJ_DEV = 256
BRICKS = 16384
TRAJECTORIES = 2048
N_MAP = 8
N_REP = 4


def draw_owners(key, part):
    per_device = TRAJ_DEV * WAYPOINTS // N_REP
    capacity = 4 * per_device // N_MAP
    remaining = per_device - capacity - capacity // 2
    even_share = remaining // (N_MAP - 2)
    leftover = remaining % (N_MAP - 2)
    places = jnp.arange(N_MAP, dtype=jnp.int32)
    quota = jnp.where(places == 0, capacity, jnp.where(places == 1, capacity // 2, even_share + (places - 2 < leftover).astype(jnp.int32)))
    limits = jnp.cumsum(quota)
    positions = jnp.arange(per_device, dtype=jnp.int32)
    which = jnp.sum((limits[None, :] <= positions[:, None]).astype(jnp.int32), axis=1)

    def one_block(block_key):
        first_key, second_key = jax.random.split(block_key)
        labels = jax.random.permutation(first_key, places)
        return jax.random.permutation(second_key, labels[which])
    block_keys = jax.random.split(jax.random.fold_in(key, 17), N_MAP * N_REP)
    blocks = jax.vmap(one_block)(block_keys).reshape(N_MAP, N_REP, TRAJ_DEV, WAYPOINTS // N_REP)
    return blocks.transpose(0, 2, 1, 3).reshape(N_MAP * TRAJ_DEV, WAYPOINTS).astype(jnp.int32)


def place_ends(result, own_key, least, top_value):
    longest = result.shape.index(max(result.shape))
    spots = []
    for shift in (0, 1):
        where = [jax.random.randint(jax.random.fold_in(own_key, axis), (), 0, length) for axis, length in enumerate(result.shape)]
        where[longest] = (where[longest] + shift) % result.shape[longest]
        spots.append(tuple(where))
    return result.at[spots[0]].set(least).at[spots[1]].set(top_value)


def steps_of(rng, shape, cuts, smallest, top_value):
    def one(position, shards_of):
        heights = jax.random.uniform(jax.random.fold_in(jax.random.fold_in(rng, 6), position), (shards_of,), jnp.float32, smallest / len(cuts), top_value / len(cuts))
        return jnp.repeat(jnp.exp(heights), shape[position] // shards_of).reshape((-1,) + (1,) * (len(shape) - position - 1))

    level = one(*cuts[0])
    for cut in cuts[1:]:
        level = level * one(*cut)
    return level


def normal_values(key, extent, deviation, reach, pieces=(), kind=jnp.bfloat16):
    values = jax.random.normal(key, extent, jnp.float32) * deviation
    if len(pieces) > 0:
        values = steps_of(key, extent, pieces, -0.22, 0.18) * values
    return jnp.clip(values, min=-reach, max=reach).astype(kind)


def setup_inputs(seed: int = 0) -> dict:
    seeds = jax.random.split(jax.random.key(seed), 6)
    field_bricks = normal_values(seeds[0], (BRICKS, VOXELS), 1.0, 6.0, ((0, 8),))
    owners = draw_owners(jax.random.fold_in(seeds[5], 71), 0)
    bricks = place_ends(jax.random.randint(seeds[2], (TRAJECTORIES, WAYPOINTS), 0, BRICK_DEV), jax.random.fold_in(seeds[2], 1), 0, BRICK_DEV - 1).astype(jnp.int32)
    corners = place_ends(jax.random.randint(seeds[3], (TRAJECTORIES, WAYPOINTS), 0, 343), jax.random.fold_in(seeds[3], 1), 0, 342).astype(jnp.int32)
    fraction = jnp.clip(1.0 * jax.random.uniform(seeds[4], (3, TRAJECTORIES, WAYPOINTS), jnp.float32) ** steps_of(seeds[4], (3, TRAJECTORIES, WAYPOINTS), ((1, 8), (2, 4)), -0.2, 0.2), 0.0, 1.0)
    return dict(field_bricks=field_bricks, owners=owners, bricks=bricks, corners=corners, fraction=fraction)


margin = 0.5


def corner_offset(corners):
    return (corners // 49) * 64 + ((corners // 7) % 7) * 8 + corners % 7


def lookup(slab_flat, cell_code, frac_x, frac_y, frac_z, stack_axis):
    total = jnp.zeros(frac_x.shape, jnp.float32)
    slope_x = jnp.zeros(frac_x.shape, jnp.float32)
    slope_y = jnp.zeros(frac_x.shape, jnp.float32)
    slope_z = jnp.zeros(frac_x.shape, jnp.float32)
    for step_x in (0, 1):
        weight_x = frac_x if step_x else 1.0 - frac_x
        sign_x = 1.0 if step_x else -1.0
        for step_y in (0, 1):
            weight_y = frac_y if step_y else 1.0 - frac_y
            sign_y = 1.0 if step_y else -1.0
            for step_z in (0, 1):
                weight_z = frac_z if step_z else 1.0 - frac_z
                sign_z = 1.0 if step_z else -1.0
                value = slab_flat[cell_code + (step_x * 64 + step_y * 8 + step_z)].astype(jnp.float32)
                total = total + weight_x * weight_y * weight_z * value
                slope_x = slope_x + sign_x * weight_y * weight_z * value
                slope_y = slope_y + sign_y * weight_x * weight_z * value
                slope_z = slope_z + sign_z * weight_x * weight_y * value
    return jnp.stack([total, slope_x, slope_y, slope_z], axis=stack_axis)


def reference(field_bricks, owners, bricks, corners, fraction):
    slab_flat = field_bricks.reshape(-1)
    cell_code = ((owners * BRICK_DEV + bricks) * 512 + corner_offset(corners)).astype(jnp.int32)
    answers = lookup(slab_flat, cell_code, fraction[0], fraction[1], fraction[2], 0)
    hinge_term = jnp.maximum(margin - answers[0], 0.0)
    trajectory_cost = jnp.sum(hinge_term * hinge_term, axis=1)
    waypoint_grad = -2.0 * hinge_term[None] * answers[1:]
    return trajectory_cost, waypoint_grad
```

```python
import functools

import jax
import jax.numpy as jnp
from jax import lax
from jax.experimental import pallas as pl
from jax.experimental.pallas import tpu as pltpu
from jax.sharding import PartitionSpec as P

margin = 0.5
LANES = 128
VMEM = pltpu.VMEM
SMEM = pltpu.SMEM


MESH = pl.DeviceIdType.MESH


def lanes_of(x):
    return jnp.concatenate(
        [x[:, h * LANES : (h + 1) * LANES] for h in range(x.shape[1] // LANES)], axis=0
    )


def iota(shape, axis):
    return lax.broadcasted_iota(jnp.int32, shape, axis)


def stay(x):
    return pltpu.with_memory_space_constraint(x, pltpu.HBM)


def each(count, body, unrolled):
    if count <= unrolled:
        for i in range(count):
            body(i)
    else:
        lax.fori_loop(0, count, lambda i, z: (body(i), z)[1], 0)


def dispatch_kernel(
    devices, tiles, owners_hbm, bricks_hbm, corners_hbm, frac_hbm,
    out_ref, own_ref, rank_ref, meta_ref,
    data_ref, pos_ref, meta_s, sem, owners_ref, bricks_ref, corners_ref, frac_ref, load_sem,
):
    loads = [
        pltpu.make_async_copy(source, target, load_sem.at[i])
        for i, (source, target) in enumerate(
            [(owners_hbm, owners_ref), (bricks_hbm, bricks_ref),
             (corners_hbm, corners_ref), (frac_hbm, frac_ref)]
        )
    ]
    for load in loads:
        load.start()
    out_ref[...] = jnp.zeros_like(out_ref)
    for load in loads:
        load.wait()
    own = lanes_of(owners_ref[...])
    chunks = own.shape[0]
    bricks = bricks_ref[...]
    corners = corners_ref[...]
    cx = (corners * 1338) >> 16
    cxy = (corners * 9363) >> 16
    code = bricks * 512 + cx * 64 + (cxy - cx * 7) * 8 + (corners - cxy * 7)
    code = lanes_of(code.astype(jnp.float32))
    for k in range(2):
        data_ref[:, 4 * k, :] = code
    for f in range(3):
        part = lanes_of(frac_ref[f])
        for k in range(2):
            data_ref[:, 4 * k + 1 + f, :] = part
    own_ref[...] = own

    upper = (iota((LANES, LANES), 0) <= iota((LANES, LANES), 1)).astype(jnp.float32).astype(jnp.bfloat16)
    ones = jnp.ones((LANES, LANES), jnp.bfloat16)
    before = (iota((chunks, chunks), 0) > iota((chunks, chunks), 1)).astype(jnp.float32).astype(jnp.bfloat16)
    lane = iota((chunks, LANES), 1)
    rank = jnp.zeros((chunks, LANES), jnp.float32)
    pos = jnp.zeros((chunks, LANES), jnp.float32)
    start = jnp.zeros((chunks, LANES), jnp.float32)
    meta = jnp.zeros((chunks, LANES), jnp.int32)
    for o in range(devices):
        member = own == o
        m16 = member.astype(jnp.float32).astype(jnp.bfloat16)
        incl = jnp.dot(m16, upper, preferred_element_type=jnp.float32) - 1.0
        total = jnp.dot(m16, ones, preferred_element_type=jnp.float32)
        off = jnp.dot(before, total.astype(jnp.bfloat16), preferred_element_type=jnp.float32)
        rank = jnp.where(member, incl + off, rank)
        pos = jnp.where(member, incl + start, pos)
        meta = jnp.where(lane == o, off.astype(jnp.int32), meta)
        turn = (off - start).astype(jnp.int32) & (LANES - 1)
        meta = jnp.where(lane == devices + o, turn, meta)
        start = start + total
        last = (off + total)[chunks - 1 : chunks, :]
        out_ref[o, 4 * tiles : 4 * tiles + 8, :] = jnp.broadcast_to(last, (8, LANES))
    rank_ref[...] = rank.astype(jnp.int32)
    pos_ref[...] = pos.astype(jnp.int32)
    meta_ref[...] = meta
    copy = pltpu.make_async_copy(meta_ref, meta_s, sem)
    copy.start()

    def sort_chunk(c):
        hot = (iota((LANES, LANES), 0) == pos_ref[pl.ds(c, 1), :]).astype(jnp.float32).astype(jnp.bfloat16)
        items = iota((8, LANES), 1).astype(jnp.float32).astype(jnp.bfloat16)
        inverse = lax.dot_general(
            items, hot, (((1,), (1,)), ((), ())), preferred_element_type=jnp.float32
        ).astype(jnp.int32)
        data_ref[c] = jnp.take_along_axis(data_ref[c], inverse, axis=1, mode="promise_in_bounds")

    for c in range(chunks):
        sort_chunk(c)
    copy.wait()
    sub8 = iota((8, LANES), 0)
    lane8 = iota((8, LANES), 1)

    def place_chunk(c, carry):
        row = data_ref[c]

        def place(o):
            off = meta_s[c, o]
            where_to = pl.ds(4 * (off >> 7), 8)
            turned = pltpu.roll(row, meta_s[c, devices + o], 1)
            keep = (sub8 < 4) & (lane8 < (off & (LANES - 1)))
            out_ref[o, where_to, :] = jnp.where(keep, out_ref[o, where_to, :], turned)

        each(devices, place, 8)
        return carry

    counts = [out_ref[o, 4 * tiles : 4 * tiles + 8, :] for o in range(devices)] if devices <= 8 else None
    if counts is None:
        last_off = meta_ref
    lax.fori_loop(0, chunks, place_chunk, 0, unroll=4 if devices <= 8 else 1)
    for o in range(devices):
        if counts is not None:
            out_ref[o, 4 * tiles : 4 * tiles + 8, :] = counts[o]
        else:
            n = meta_s[chunks - 1, o] + jnp.sum((own_ref[chunks - 1 : chunks, :] == o).astype(jnp.int32))
            out_ref[o, 4 * tiles : 4 * tiles + 8, :] = jnp.full((8, LANES), n, jnp.int32).astype(jnp.float32)


def lookup_kernel(
    devices, tiles, table, in_ref, out_ref, index_v, index_s, rows_a, rows_b, sem
):
    span = tiles + 1
    bricks = table.shape[0] // 7
    for s in range(devices):
        codes = in_ref[s, pl.ds(0, span, stride=4), :].astype(jnp.int32)
        is_count = iota((span, LANES), 0) == tiles
        row = ((codes >> 6) & 7) * bricks + (codes >> 9)
        used = jnp.maximum((codes + LANES - 1) >> 7, 1)
        index_v[pl.ds(s * span, span), :] = jnp.where(is_count, used, row)
    copy = pltpu.make_async_copy(index_v, index_s, sem)
    copy.start()
    copy.wait()
    sub8 = iota((8, LANES), 0)

    def used_of(s):
        return index_s[s * span + tiles, 0]

    def following(s, t):
        more = t + 1 < used_of(s)
        last = s + 1 >= devices
        t_next = jnp.where(more, t + 1, jnp.where(last, t, 0))
        s_next = jnp.where(more | last, s, s + 1)
        return s_next, t_next

    def gather(s, t, rows):
        line = index_s.at[s * span + t]
        for p in range(LANES):
            rows[p : p + 1, :] = table[pl.ds(line[p], 1), :]

    def weigh(s, t, rows):
        cells = rows[...].T
        query = in_ref[s, pl.ds(4 * t, 4), :]
        code = query[0:1].astype(jnp.int32)
        cy = jnp.broadcast_to((code >> 3) & 7, (8, LANES))
        cz = jnp.broadcast_to(code & 7, (8, LANES))
        fx = jnp.broadcast_to(query[1:2], (8, LANES))
        fy = jnp.broadcast_to(query[2:3], (8, LANES))
        fz = jnp.broadcast_to(query[3:4], (8, LANES))
        zero = jnp.zeros((8, LANES), jnp.float32)
        inter = [zero, zero]
        slope = [zero, zero]
        for y in range(8):
            low, high = cy == y, cy == y - 1
            weight = jnp.where(low, 1.0 - fy, jnp.where(high, fy, 0.0))
            sign = jnp.where(low, -1.0, jnp.where(high, 1.0, 0.0))
            for a in range(2):
                v = cells[64 * a + 8 * y : 64 * a + 8 * y + 8, :]
                inter[a] = inter[a] + weight * v
                slope[a] = slope[a] + sign * v
        low, high = cz == sub8, cz == sub8 - 1
        weight = jnp.where(low, 1.0 - fz, jnp.where(high, fz, 0.0))
        sign = jnp.where(low, -1.0, jnp.where(high, 1.0, 0.0))
        mixed = (1.0 - fx) * inter[0] + fx * inter[1]
        parts = [
            weight * mixed,
            weight * (inter[1] - inter[0]),
            weight * ((1.0 - fx) * slope[0] + fx * slope[1]),
            sign * mixed,
        ]
        out_ref[s, pl.ds(4 * t, 4), :] = jnp.concatenate(
            [jnp.sum(q, axis=0, keepdims=True) for q in parts], axis=0
        )

    total = used_of(0)
    for s in range(1, devices):
        total = total + used_of(s)

    def pair(i, now):
        s0, t0 = now
        s1, t1 = following(s0, t0)
        s2, t2 = following(s1, t1)
        gather(s1, t1, rows_b)
        weigh(s0, t0, rows_a)
        gather(s2, t2, rows_a)
        weigh(s1, t1, rows_b)
        return s2, t2

    first = (jnp.int32(0), jnp.int32(0))
    gather(*first, rows_a)
    lax.fori_loop(0, (total + 1) >> 1, pair, first)


def greet(peers):
    barrier = pltpu.get_barrier_semaphore()
    for peer in peers:
        pl.semaphore_signal(barrier, inc=1, device_id=peer, device_id_type=MESH)
    pl.semaphore_wait(barrier, len(peers))


def peer_along(axis, size, step):
    return {axis: lax.rem(lax.axis_index(axis) + step, size)}


def starts(devices, lines, src_ref, dst_of, send_sem, recv_sem):
    me = lax.axis_index("map")
    copies = []
    for k in range(1, devices):
        to = lax.rem(me + k, devices)
        copy = pltpu.make_async_remote_copy(
            src_ref=src_ref.at[to, pl.ds(0, lines)],
            dst_ref=dst_of(k),
            send_sem=send_sem.at[k],
            recv_sem=recv_sem.at[k],
            device_id={"map": to},
            device_id_type=MESH,
        )
        copy.start()
        copies.append(copy)
    own = pltpu.make_async_copy(
        src_ref.at[me, pl.ds(0, lines)], dst_of(0), recv_sem.at[0]
    )
    own.start()
    return own, copies


def exchange_kernel(devices, lines, in_ref, field_hbm, out_ref, table, send_sem, recv_sem, field_ref, field_sem):
    load = pltpu.make_async_copy(field_hbm, field_ref, field_sem)
    load.start()
    greet([peer_along("map", devices, k) for k in range(1, devices)])
    me = lax.axis_index("map")
    own, copies = starts(
        devices, lines, in_ref, lambda k: out_ref.at[me, pl.ds(0, lines)], send_sem, recv_sem
    )
    bricks = field_ref.shape[0]

    def build(g, carry):
        block = field_ref[pl.ds(pl.multiple_of(g * 16, 16), 16), :].astype(jnp.float32)
        for x in range(7):
            table[pl.ds(pl.multiple_of(x * bricks + g * 16, 16), 16), :] = block[:, 64 * x : 64 * x + 128]
        return carry

    load.wait()
    lax.fori_loop(0, bricks // 16, build, 0, unroll=8)
    own.wait()
    for copy in copies:
        copy.wait()


def combine_kernel(
    devices, reps, lines, in_ref, own_ref, rank_ref, meta_s, cost_ref, grad_ref,
    held, costs, send_sem, recv_sem, cost_send, cost_recv, *landed,
):
    greet(
        [peer_along("map", devices, k) for k in range(1, devices)]
        + [peer_along("rep", reps, k) for k in range(1, reps)]
    )
    own_copy, copies = starts(
        devices, lines, in_ref, lambda k: landed[k].at[pl.ds(0, lines)], send_sem, recv_sem
    )
    me = lax.axis_index("map")
    chunks = own_ref.shape[0]
    sub8 = iota((8, LANES), 0)
    half = (sub8 >= 4).astype(jnp.int32)
    own_copy.wait()
    for copy in copies:
        copy.wait_recv()

    def chunk(c, carry):
        owner = jnp.broadcast_to(own_ref[pl.ds(c, 1), :], (8, LANES))
        rank = jnp.broadcast_to(rank_ref[pl.ds(c, 1), :], (8, LANES))
        lane = rank & (LANES - 1)
        which = (rank >> 7) - half
        value = jnp.zeros((8, LANES), jnp.float32)
        for k in range(devices):
            source = lax.rem(me + devices - k, devices)
            w = meta_s[c, source] >> 7
            picked = jnp.take_along_axis(
                landed[k][pl.ds(4 * w, 8), :], lane, axis=1, mode="promise_in_bounds"
            )
            value = jnp.where((owner == source) & (which == w), picked, value)
        held[c] = value
        return carry

    lax.fori_loop(0, chunks, chunk, 0, unroll=4 if devices <= 8 else 1)
    dist = held[:, 0, :] + held[:, 4, :]
    hinge = jnp.maximum(margin - dist, 0.0)
    halves = grad_ref.shape[2] // LANES
    quarter = chunks // halves
    for h in range(halves):
        here = hinge[h * quarter : (h + 1) * quarter]
        costs[0, :, h * LANES : (h + 1) * LANES] = jnp.sum(here * here, axis=0, keepdims=True)
    sums = []
    for k in range(1, reps):
        copy = pltpu.make_async_remote_copy(
            src_ref=costs.at[0],
            dst_ref=costs.at[k],
            send_sem=cost_send.at[k],
            recv_sem=cost_recv.at[k],
            device_id=peer_along("rep", reps, k),
            device_id_type=MESH,
        )
        copy.start()
        sums.append(copy)
    for n in range(3):
        grad = -2.0 * hinge * (held[:, 1 + n, :] + held[:, 5 + n, :])
        for h in range(halves):
            grad_ref[n, :, h * LANES : (h + 1) * LANES] = grad[h * quarter : (h + 1) * quarter]
    for copy in copies:
        copy.wait_send()
    total = costs[0]
    for k, copy in enumerate(sums):
        copy.wait()
        total = total + costs[k + 1]
    cost_ref[...] = total


def finish_kernel(cost_in, grad_in, cost_out, grad_out, sem):
    copies = [
        pltpu.make_async_copy(grad_in, grad_out, sem.at[0]),
        pltpu.make_async_copy(cost_in, cost_out, sem.at[1]),
    ]
    for copy in copies:
        copy.start()
    for copy in copies:
        copy.wait()


def per_device(field_bricks, owners, bricks, corners, fraction):
    devices = lax.axis_size("map")
    trajectories_here, quarter = owners.shape
    row_count = trajectories_here * quarter
    capacity = 4 * row_count // devices
    tiles = -(-capacity // LANES)
    chunks = row_count // LANES
    lines = -(-(4 * tiles + 8) // 8) * 8
    buffer = jax.ShapeDtypeStruct((devices, lines, LANES), jnp.float32)
    flat = jax.ShapeDtypeStruct((chunks, LANES), jnp.int32)
    vm = pl.BlockSpec(memory_space=VMEM)
    sm = pl.BlockSpec(memory_space=SMEM)
    hbm = pl.BlockSpec(memory_space=pltpu.HBM)
    whole = VMEM((quarter, trajectories_here), jnp.int32)
    outgoing, own, rank, meta = pl.pallas_call(
        functools.partial(dispatch_kernel, devices, tiles),
        out_shape=(buffer, flat, flat, flat),
        in_specs=[hbm] * 4,
        out_specs=(vm,) * 4,
        scratch_shapes=[
            VMEM((chunks, 8, LANES), jnp.float32),
            VMEM((chunks, LANES), jnp.int32),
            SMEM((chunks, LANES), jnp.int32),
            pltpu.SemaphoreType.DMA(()),
            whole, whole, whole,
            VMEM((3, quarter, trajectories_here), jnp.float32),
            pltpu.SemaphoreType.DMA((4,)),
        ],
        compiler_params=pltpu.CompilerParams(vmem_limit_bytes=16 << 20),
        name="dispatch",
    )(*(stay(x) for x in (owners.T, bricks.T, corners.T, fraction.transpose(0, 2, 1))))
    span = tiles + 1
    sems = pltpu.SemaphoreType.DMA((devices,))
    table = VMEM((field_bricks.shape[0] * 7, LANES), jnp.float32)
    incoming, table = pl.pallas_call(
        functools.partial(exchange_kernel, devices, 4 * span),
        out_shape=(buffer, table),
        in_specs=[vm, hbm],
        out_specs=(vm, vm),
        scratch_shapes=[
            sems, sems, VMEM(field_bricks.shape, field_bricks.dtype), pltpu.SemaphoreType.DMA(()),
        ],
        compiler_params=pltpu.CompilerParams(collective_id=0, has_side_effects=True, vmem_limit_bytes=16 << 20),
        name="send_queries",
    )(outgoing, stay(field_bricks))
    located = pl.pallas_call(
        functools.partial(lookup_kernel, devices, tiles),
        out_shape=buffer,
        in_specs=[vm] * 2,
        out_specs=vm,
        scratch_shapes=[
            VMEM((devices * span, LANES), jnp.int32),
            SMEM((devices * span, LANES), jnp.int32),
            VMEM((LANES, LANES), jnp.float32),
            VMEM((LANES, LANES), jnp.float32),
            pltpu.SemaphoreType.DMA(()),
        ],
        compiler_params=pltpu.CompilerParams(vmem_limit_bytes=16 << 20),
        name="lookup",
    )(table, incoming)
    reps = lax.axis_size("rep")
    rep_sems = pltpu.SemaphoreType.DMA((reps,))
    cost, waypoint_grad = pl.pallas_call(
        functools.partial(combine_kernel, devices, reps, 4 * tiles),
        out_shape=(
            jax.ShapeDtypeStruct((1, trajectories_here), jnp.float32),
            jax.ShapeDtypeStruct((3, quarter, trajectories_here), jnp.float32),
        ),
        in_specs=[vm, vm, vm, sm],
        out_specs=(vm, vm),
        scratch_shapes=[
            VMEM((chunks, 8, LANES), jnp.float32),
            VMEM((reps, 1, trajectories_here), jnp.float32),
            sems, sems, rep_sems, rep_sems,
        ]
        + [VMEM((lines, LANES), jnp.float32)] * devices,
        compiler_params=pltpu.CompilerParams(collective_id=1, has_side_effects=True, vmem_limit_bytes=16 << 20),
        name="combine",
    )(located, own, rank, meta)
    cost, waypoint_grad = pl.pallas_call(
        finish_kernel,
        out_shape=(
            jax.ShapeDtypeStruct(cost.shape, jnp.float32),
            jax.ShapeDtypeStruct(waypoint_grad.shape, jnp.float32),
        ),
        in_specs=[vm] * 2,
        out_specs=(hbm,) * 2,
        scratch_shapes=[pltpu.SemaphoreType.DMA((2,))],
        compiler_params=pltpu.CompilerParams(vmem_limit_bytes=1 << 20),
        name="finish",
    )(cost, waypoint_grad)
    return cost.reshape(trajectories_here), waypoint_grad.transpose(0, 2, 1)


def solution(mesh):
    placed = (
        P("map", None),
        P("map", "rep"),
        P("map", "rep"),
        P("map", "rep"),
        P(None, "map", "rep"),
    )
    return jax.shard_map(
        per_device,
        mesh=mesh,
        in_specs=placed,
        out_specs=(P("map"), P(None, "map", "rep")),
        check_vma=False,
    )
```

```python
import functools

import jax
import jax.numpy as jnp
from jax import lax
from jax.experimental import pallas as pl
from jax.experimental.pallas import tpu as pltpu
from jax.sharding import PartitionSpec as P

margin = 0.5
LANES = 128
VMEM = pltpu.VMEM
SMEM = pltpu.SMEM


MESH = pl.DeviceIdType.MESH


def lanes_of(x):
    return jnp.concatenate(
        [x[:, h * LANES : (h + 1) * LANES] for h in range(x.shape[1] // LANES)], axis=0
    )


def iota(shape, axis):
    return lax.broadcasted_iota(jnp.int32, shape, axis)


def stay(x):
    return pltpu.with_memory_space_constraint(x, pltpu.HBM)


def each(count, body, unrolled):
    if count <= unrolled:
        for i in range(count):
            body(i)
    else:
        lax.fori_loop(0, count, lambda i, z: (body(i), z)[1], 0)


def dispatch_kernel(
    devices, tiles, owners_hbm, bricks_hbm, corners_hbm, frac_hbm,
    out_ref, own_ref, rank_ref, meta_ref,
    data_ref, pos_ref, meta_s, sem, owners_ref, bricks_ref, corners_ref, frac_ref, load_sem,
):
    loads = [
        pltpu.make_async_copy(source, target, load_sem.at[i])
        for i, (source, target) in enumerate(
            [(owners_hbm, owners_ref), (bricks_hbm, bricks_ref),
             (corners_hbm, corners_ref), (frac_hbm, frac_ref)]
        )
    ]
    for load in loads:
        load.start()
    out_ref[...] = jnp.zeros_like(out_ref)
    for load in loads:
        load.wait()
    own = lanes_of(owners_ref[...])
    chunks = own.shape[0]
    bricks = bricks_ref[...]
    corners = corners_ref[...]
    cx = (corners * 1338) >> 16
    cxy = (corners * 9363) >> 16
    code = bricks * 512 + cx * 64 + (cxy - cx * 7) * 8 + (corners - cxy * 7)
    code = lanes_of(code.astype(jnp.float32))
    for k in range(2):
        data_ref[:, 4 * k, :] = code
    for f in range(3):
        part = lanes_of(frac_ref[f])
        for k in range(2):
            data_ref[:, 4 * k + 1 + f, :] = part
    own_ref[...] = own

    upper = (iota((LANES, LANES), 0) <= iota((LANES, LANES), 1)).astype(jnp.float32).astype(jnp.bfloat16)
    ones = jnp.ones((LANES, LANES), jnp.bfloat16)
    before = (iota((chunks, chunks), 0) > iota((chunks, chunks), 1)).astype(jnp.float32).astype(jnp.bfloat16)
    lane = iota((chunks, LANES), 1)
    rank = jnp.zeros((chunks, LANES), jnp.float32)
    pos = jnp.zeros((chunks, LANES), jnp.float32)
    start = jnp.zeros((chunks, LANES), jnp.float32)
    meta = jnp.zeros((chunks, LANES), jnp.int32)
    for o in range(devices):
        member = own == o
        m16 = member.astype(jnp.float32).astype(jnp.bfloat16)
        incl = jnp.dot(m16, upper, preferred_element_type=jnp.float32) - 1.0
        total = jnp.dot(m16, ones, preferred_element_type=jnp.float32)
        off = jnp.dot(before, total.astype(jnp.bfloat16), preferred_element_type=jnp.float32)
        rank = jnp.where(member, incl + off, rank)
        pos = jnp.where(member, incl + start, pos)
        meta = jnp.where(lane == o, off.astype(jnp.int32), meta)
        turn = (off - start).astype(jnp.int32) & (LANES - 1)
        meta = jnp.where(lane == devices + o, turn, meta)
        start = start + total
    rank_ref[...] = rank.astype(jnp.int32)
    pos_ref[...] = pos.astype(jnp.int32)
    meta_ref[...] = meta
    copy = pltpu.make_async_copy(meta_ref, meta_s, sem)
    copy.start()

    def sort_chunk(c):
        hot = (iota((LANES, LANES), 0) == pos_ref[pl.ds(c, 1), :]).astype(jnp.float32).astype(jnp.bfloat16)
        items = iota((8, LANES), 1).astype(jnp.float32).astype(jnp.bfloat16)
        inverse = lax.dot_general(
            items, hot, (((1,), (1,)), ((), ())), preferred_element_type=jnp.float32
        ).astype(jnp.int32)
        data_ref[c] = jnp.take_along_axis(data_ref[c], inverse, axis=1, mode="promise_in_bounds")

    for c in range(chunks):
        sort_chunk(c)
    copy.wait()
    sub8 = iota((8, LANES), 0)
    lane8 = iota((8, LANES), 1)

    def place_chunk(c, carry):
        row = data_ref[c]

        def place(o):
            off = meta_s[c, o]
            where_to = pl.ds(4 * (off >> 7), 8)
            turned = pltpu.roll(row, meta_s[c, devices + o], 1)
            keep = (sub8 < 4) & (lane8 < (off & (LANES - 1)))
            out_ref[o, where_to, :] = jnp.where(keep, out_ref[o, where_to, :], turned)

        each(devices, place, 8)
        return carry

    lax.fori_loop(0, chunks, place_chunk, 0, unroll=4 if devices <= 8 else 1)


def greet(peers):
    barrier = pltpu.get_barrier_semaphore()
    for peer in peers:
        pl.semaphore_signal(barrier, inc=1, device_id=peer, device_id_type=MESH)
    return lambda: pl.semaphore_wait(barrier, len(peers))


def peer_along(axis, size, step):
    return {axis: lax.rem(lax.axis_index(axis) + step, size)}


def batch_of(tiles):
    return max(n for n in (4, 2, 1) if (tiles // 2) % n == 0)


def fused_kernel(
    devices, reps, tiles, out_in, field_hbm, own_ref, rank_ref, meta_ref, cost_ref, grad_ref,
    meta_s, table, field_ref, incoming, answers, landed, landed_last, index_v, index_s, rows, cells, held, costs,
    field_sem, meta_sem, index_sem, query_send, query_recv, answer_send, answer_recv, cost_send, cost_recv,
):
    lines = 4 * tiles
    pairs = tiles // 2
    total = devices * pairs
    batch = batch_of(tiles)
    batches = pairs // batch
    bricks = field_ref.shape[0]
    me = lax.axis_index("map")
    load = pltpu.make_async_copy(field_hbm, field_ref, field_sem)
    load.start()
    meta_copy = pltpu.make_async_copy(meta_ref, meta_s, meta_sem)
    meta_copy.start()
    wait_peers = greet(
        [peer_along("map", devices, k) for k in range(1, devices)]
        + [peer_along("rep", reps, k) for k in range(1, reps)]
    )

    def ahead(k):
        return lax.rem(me + k, devices)

    def behind(k):
        return lax.rem(me + devices - k, devices)

    def query_copy(k):
        return pltpu.make_async_remote_copy(
            src_ref=out_in.at[ahead(k), pl.ds(0, lines)],
            dst_ref=incoming.at[pl.ds(pl.multiple_of(k * lines, 8), lines)],
            send_sem=query_send.at[k],
            recv_sem=query_recv.at[k],
            device_id={"map": ahead(k)},
            device_id_type=MESH,
        )

    def answer_copy(k, last=False):
        return pltpu.make_async_remote_copy(
            src_ref=answers.at[pl.ds(pl.multiple_of(k * lines, 8), lines)],
            dst_ref=(landed_last if last else landed.at[k]).at[pl.ds(0, lines)],
            send_sem=answer_send.at[k],
            recv_sem=answer_recv.at[k],
            device_id={"map": behind(k)},
            device_id_type=MESH,
        )

    incoming[0:lines] = out_in[me, 0:lines]
    rows[...] = jnp.zeros_like(rows)
    cells[...] = jnp.zeros_like(cells)

    def build(g, carry):
        block = field_ref[pl.ds(pl.multiple_of(g * 16, 16), 16), :].astype(jnp.float32)
        for x in range(7):
            table[pl.ds(pl.multiple_of(x * bricks + g * 16, 16), 16), :] = block[:, 64 * x : 64 * x + 128]
        return carry

    wait_peers()
    each(devices - 1, lambda k: query_copy(k + 1).start(), 8)
    load.wait()
    lax.fori_loop(0, bricks // 16, build, 0, unroll=32)

    def index_copy(slot):
        return pltpu.make_async_copy(index_v.at[slot], index_s.at[slot], index_sem.at[slot])

    def start_index(j, slot):
        first = pl.multiple_of(j * (8 * batch), 8)
        codes = incoming[pl.ds(first, 2 * batch, stride=4), :].astype(jnp.int32)
        row = ((codes >> 6) & 7) * bricks + (codes >> 9)
        index_v[slot] = jnp.clip(row, 0, 7 * bricks - 1)
        index_copy(slot).start()

    sub8 = iota((8, LANES), 0)

    def gather(slot, pair):
        for half in range(2):
            for p in range(LANES):
                rows[half, p : p + 1, :] = table[pl.ds(index_s[slot, 2 * pair + half, p], 1), :]

    def turn():
        for half in range(2):
            cells[half] = rows[half].T

    def weigh(g):
        query = incoming[pl.ds(pl.multiple_of(8 * g, 8), 8), :]
        code = query.astype(jnp.int32)
        results = []
        for half in range(2):
            row = 4 * half
            cy = jnp.broadcast_to((code[row : row + 1] >> 3) & 7, (8, LANES))
            cz = jnp.broadcast_to(code[row : row + 1] & 7, (8, LANES))
            fx = jnp.broadcast_to(query[row + 1 : row + 2], (8, LANES))
            fy = jnp.broadcast_to(query[row + 2 : row + 3], (8, LANES))
            fz = jnp.broadcast_to(query[row + 3 : row + 4], (8, LANES))
            is_y = [cy == y for y in range(7)]
            inter, slope = [], []
            for a in range(2):
                v = [cells[half, 64 * a + 8 * y : 64 * a + 8 * y + 8, :] for y in range(8)]
                low, high = v[0], v[1]
                for y in range(1, 7):
                    low = jnp.where(is_y[y], v[y], low)
                    high = jnp.where(is_y[y], v[y + 1], high)
                inter.append((1.0 - fy) * low + fy * high)
                slope.append(high - low)
            low, high = cz == sub8, cz == sub8 - 1
            weight = jnp.where(low, 1.0 - fz, jnp.where(high, fz, 0.0))
            sign = jnp.where(low, -1.0, jnp.where(high, 1.0, 0.0))
            mixed = (1.0 - fx) * inter[0] + fx * inter[1]
            results += [
                weight * mixed,
                weight * (inter[1] - inter[0]),
                weight * ((1.0 - fx) * slope[0] + fx * slope[1]),
                sign * mixed,
            ]
        for step in (4, 2, 1):
            upper = (sub8 & step) == 0
            count = len(results) // 2
            results = [
                jnp.where(upper, results[i], pltpu.roll(results[i + count], step, 0))
                + jnp.where(upper, pltpu.roll(results[i], 8 - step, 0), results[i + count])
                for i in range(count)
            ]
        answers[pl.ds(pl.multiple_of(8 * g, 8), 8), :] = results[0]

    def step(g, slot, pair):
        weigh(jnp.maximum(g - 2, 0))
        turn()
        if slot is not None:
            gather(slot, pair)

    def finished(j):
        return ((j + 1) * batch + pairs - 2) // pairs - 1

    def segment(j, slot):
        following = j + 1
        source = following // batches

        def prepare():
            if batches == 1 or slot == 1:

                @pl.when(source < devices)
                def _():
                    query_copy(source).wait_recv()

            @pl.when(following < devices * batches)
            def _():
                start_index(following, 1 - slot)

        pl.when(source != 1)(prepare) if batches == 1 or slot == 1 else prepare()
        index_copy(slot).wait()
        for p in range(batch):
            step(j * batch + p, slot, p)
        if batches == 1 or slot == 1:
            pl.when(source == 1)(prepare)
        done = finished(j)

        @pl.when((done > finished(j - 1)) & (done > 1))
        def _():
            answer_copy(done - 1).start()

    def double(i, carry):
        segment(2 * i, 0)
        segment(2 * i + 1, 1)
        return carry

    count = devices * batches
    start_index(0, 0)
    lax.fori_loop(0, count // 2, double, 0)
    step(total, None, None)
    step(total + 1, None, None)
    for k in range(max(finished(count - 1), 1), devices):
        answer_copy(k, k == devices - 1).start()
    landed[0, 0:lines] = answers[0:lines]

    chunks = own_ref.shape[0]
    half = (sub8 >= 4).astype(jnp.int32)

    def collect(slots, first):
        def chunk(c, carry):
            owner = jnp.broadcast_to(own_ref[pl.ds(c, 1), :], (8, LANES))
            rank = jnp.broadcast_to(rank_ref[pl.ds(c, 1), :], (8, LANES))
            lane = rank & (LANES - 1)
            which = (rank >> 7) - half
            value = jnp.zeros((8, LANES), jnp.float32) if first else held[c]
            for k in slots:
                owner_k = ahead(k)
                w = meta_s[c, owner_k] >> 7
                where = pl.ds(4 * w, 8)
                picked = jnp.take_along_axis(
                    landed_last[where, :] if k == devices - 1 else landed[k, where, :], lane, axis=1, mode="promise_in_bounds"
                )
                value = jnp.where((owner == owner_k) & (which == w), picked, value)
            held[c] = value
            return carry

        lax.fori_loop(0, chunks, chunk, 0, unroll=4 if devices <= 8 else 1)

    meta_copy.wait()
    each(devices - 2, lambda k: answer_copy(k + 1).wait_recv(), 8)
    collect(range(devices - 1), True)
    answer_copy(devices - 1, True).wait_recv()
    collect([devices - 1], False)
    dist = held[:, 0, :] + held[:, 4, :]
    hinge = jnp.maximum(margin - dist, 0.0)
    halves = grad_ref.shape[2] // LANES
    quarter = chunks // halves
    for h in range(halves):
        here = hinge[h * quarter : (h + 1) * quarter]
        costs[0, :, h * LANES : (h + 1) * LANES] = jnp.sum(here * here, axis=0, keepdims=True)
    sums = []
    for k in range(1, reps):
        copy = pltpu.make_async_remote_copy(
            src_ref=costs.at[0],
            dst_ref=costs.at[k],
            send_sem=cost_send.at[k],
            recv_sem=cost_recv.at[k],
            device_id=peer_along("rep", reps, k),
            device_id_type=MESH,
        )
        copy.start()
        sums.append(copy)
    for n in range(3):
        grad = -2.0 * hinge * (held[:, 1 + n, :] + held[:, 5 + n, :])
        for h in range(halves):
            grad_ref[n, :, h * LANES : (h + 1) * LANES] = grad[h * quarter : (h + 1) * quarter]

    each(devices - 1, lambda k: query_copy(k + 1).wait_send(), 8)
    each(devices - 2, lambda k: answer_copy(k + 1).wait_send(), 8)
    answer_copy(devices - 1, True).wait_send()
    total_cost = costs[0]
    for k, copy in enumerate(sums):
        copy.wait()
        total_cost = total_cost + costs[k + 1]
    cost_ref[...] = total_cost


def finish_kernel(cost_in, grad_in, cost_out, grad_out, sem):
    copies = [
        pltpu.make_async_copy(grad_in, grad_out, sem.at[0]),
        pltpu.make_async_copy(cost_in, cost_out, sem.at[1]),
    ]
    for copy in copies:
        copy.start()
    for copy in copies:
        copy.wait()


def per_device(field_bricks, owners, bricks, corners, fraction):
    devices = lax.axis_size("map")
    trajectories_here, quarter = owners.shape
    row_count = trajectories_here * quarter
    capacity = 4 * row_count // devices
    tiles = 2 * -(-capacity // (2 * LANES))
    chunks = row_count // LANES
    lines = 4 * tiles
    buffer = jax.ShapeDtypeStruct((devices, lines + 8, LANES), jnp.float32)
    flat = jax.ShapeDtypeStruct((chunks, LANES), jnp.int32)
    vm = pl.BlockSpec(memory_space=VMEM)
    sm = pl.BlockSpec(memory_space=SMEM)
    hbm = pl.BlockSpec(memory_space=pltpu.HBM)
    whole = VMEM((quarter, trajectories_here), jnp.int32)
    outgoing, own, rank, meta = pl.pallas_call(
        functools.partial(dispatch_kernel, devices, tiles),
        out_shape=(buffer, flat, flat, flat),
        in_specs=[hbm] * 4,
        out_specs=(vm,) * 4,
        scratch_shapes=[
            VMEM((chunks, 8, LANES), jnp.float32),
            VMEM((chunks, LANES), jnp.int32),
            SMEM((chunks, LANES), jnp.int32),
            pltpu.SemaphoreType.DMA(()),
            whole, whole, whole,
            VMEM((3, quarter, trajectories_here), jnp.float32),
            pltpu.SemaphoreType.DMA((4,)),
        ],
        compiler_params=pltpu.CompilerParams(vmem_limit_bytes=16 << 20),
        name="dispatch",
    )(*(stay(x) for x in (owners.T, bricks.T, corners.T, fraction.transpose(0, 2, 1))))
    sems = pltpu.SemaphoreType.DMA((devices,))
    reps = lax.axis_size("rep")
    rep_sems = pltpu.SemaphoreType.DMA((reps,))
    batch = batch_of(tiles)
    square = VMEM((2, LANES, LANES), jnp.float32)
    bricks = field_bricks.shape[0]
    cost, waypoint_grad = pl.pallas_call(
        functools.partial(fused_kernel, devices, reps, tiles),
        out_shape=(
            jax.ShapeDtypeStruct((1, trajectories_here), jnp.float32),
            jax.ShapeDtypeStruct((3, quarter, trajectories_here), jnp.float32),
        ),
        in_specs=[vm, hbm, vm, vm, vm],
        out_specs=(vm, vm),
        scratch_shapes=[
            SMEM((chunks, LANES), jnp.int32),
            VMEM((bricks * 7, LANES), jnp.float32),
            VMEM(field_bricks.shape, field_bricks.dtype),
            VMEM((devices * lines, LANES), jnp.float32),
            VMEM((devices * lines, LANES), jnp.float32),
            VMEM((devices - 1, lines + 8, LANES), jnp.float32),
            VMEM((lines + 8, LANES), jnp.float32),
            VMEM((2, 2 * batch, LANES), jnp.int32),
            SMEM((2, 2 * batch, LANES), jnp.int32),
            square, square,
            VMEM((chunks, 8, LANES), jnp.float32),
            VMEM((reps, 1, trajectories_here), jnp.float32),
            pltpu.SemaphoreType.DMA(()),
            pltpu.SemaphoreType.DMA(()),
            pltpu.SemaphoreType.DMA((2,)),
            sems, sems, sems, sems, rep_sems, rep_sems,
        ],
        compiler_params=pltpu.CompilerParams(collective_id=0, has_side_effects=True, vmem_limit_bytes=24 << 20),
        name="fused",
    )(outgoing, stay(field_bricks), own, rank, meta)
    cost, waypoint_grad = pl.pallas_call(
        finish_kernel,
        out_shape=(
            jax.ShapeDtypeStruct(cost.shape, jnp.float32),
            jax.ShapeDtypeStruct(waypoint_grad.shape, jnp.float32),
        ),
        in_specs=[vm] * 2,
        out_specs=(hbm,) * 2,
        scratch_shapes=[pltpu.SemaphoreType.DMA((2,))],
        compiler_params=pltpu.CompilerParams(vmem_limit_bytes=1 << 20),
        name="finish",
    )(cost, waypoint_grad)
    return cost.reshape(trajectories_here), waypoint_grad.transpose(0, 2, 1)


def solution(mesh):
    placed = (
        P("map", None),
        P("map", "rep"),
        P("map", "rep"),
        P("map", "rep"),
        P(None, "map", "rep"),
    )
    return jax.shard_map(
        per_device,
        mesh=mesh,
        in_specs=placed,
        out_specs=(P("map"), P(None, "map", "rep")),
        check_vma=False,
    )
```

```python
import functools

import jax
import jax.numpy as jnp
from jax import lax
from jax.experimental import pallas as pl
from jax.experimental.pallas import tpu as pltpu
from jax.sharding import PartitionSpec as P

margin = 0.5
LANES = 128
VMEM = pltpu.VMEM
SMEM = pltpu.SMEM


MESH = pl.DeviceIdType.MESH


def lanes_of(x):
    return jnp.concatenate(
        [x[:, h * LANES : (h + 1) * LANES] for h in range(x.shape[1] // LANES)], axis=0
    )


def iota(shape, axis):
    return lax.broadcasted_iota(jnp.int32, shape, axis)


def stay(x):
    return pltpu.with_memory_space_constraint(x, pltpu.HBM)


def each(count, body, unrolled):
    if count <= unrolled:
        for i in range(count):
            body(i)
    else:
        lax.fori_loop(0, count, lambda i, z: (body(i), z)[1], 0)


def dispatch_kernel(
    devices, tiles, owners_hbm, bricks_hbm, corners_hbm, frac_hbm, field_hbm,
    out_ref, own_ref, rank_ref, meta_ref, field_ref,
    data_ref, pos_ref, meta_s, sem, owners_ref, bricks_ref, corners_ref, frac_ref, load_sem,
):
    loads = [
        pltpu.make_async_copy(source, target, load_sem.at[i])
        for i, (source, target) in enumerate(
            [(owners_hbm, owners_ref), (bricks_hbm, bricks_ref),
             (corners_hbm, corners_ref), (frac_hbm, frac_ref)]
        )
    ]
    for load in loads:
        load.start()
    field_load = pltpu.make_async_copy(field_hbm, field_ref, load_sem.at[4])
    field_load.start()
    out_ref[...] = jnp.zeros_like(out_ref)
    for load in loads:
        load.wait()
    own = lanes_of(owners_ref[...])
    chunks = own.shape[0]
    bricks = bricks_ref[...]
    corners = corners_ref[...]
    cx = (corners * 1338) >> 16
    cxy = (corners * 9363) >> 16
    code = bricks * 512 + cx * 64 + (cxy - cx * 7) * 8 + (corners - cxy * 7)
    code = lanes_of(code.astype(jnp.float32))
    for k in range(2):
        data_ref[:, 4 * k, :] = code
    for f in range(3):
        part = lanes_of(frac_ref[f])
        for k in range(2):
            data_ref[:, 4 * k + 1 + f, :] = part
    own_ref[...] = own

    upper = (iota((LANES, LANES), 0) <= iota((LANES, LANES), 1)).astype(jnp.float32).astype(jnp.bfloat16)
    ones = jnp.ones((LANES, LANES), jnp.bfloat16)
    before = (iota((chunks, chunks), 0) > iota((chunks, chunks), 1)).astype(jnp.float32).astype(jnp.bfloat16)
    lane = iota((chunks, LANES), 1)
    rank = jnp.zeros((chunks, LANES), jnp.float32)
    pos = jnp.zeros((chunks, LANES), jnp.float32)
    start = jnp.zeros((chunks, LANES), jnp.float32)
    meta = jnp.zeros((chunks, LANES), jnp.int32)
    for o in range(devices):
        member = own == o
        m16 = member.astype(jnp.float32).astype(jnp.bfloat16)
        incl = jnp.dot(m16, upper, preferred_element_type=jnp.float32) - 1.0
        total = jnp.dot(m16, ones, preferred_element_type=jnp.float32)
        off = jnp.dot(before, total.astype(jnp.bfloat16), preferred_element_type=jnp.float32)
        rank = jnp.where(member, incl + off, rank)
        pos = jnp.where(member, incl + start, pos)
        meta = jnp.where(lane == o, off.astype(jnp.int32), meta)
        turn = (off - start).astype(jnp.int32) & (LANES - 1)
        meta = jnp.where(lane == devices + o, turn, meta)
        start = start + total
    rank_ref[...] = rank.astype(jnp.int32)
    pos_ref[...] = pos.astype(jnp.int32)
    meta_ref[...] = meta
    copy = pltpu.make_async_copy(meta_ref, meta_s, sem)
    copy.start()

    def sort_chunk(c):
        hot = (iota((LANES, LANES), 0) == pos_ref[pl.ds(c, 1), :]).astype(jnp.float32).astype(jnp.bfloat16)
        items = iota((8, LANES), 1).astype(jnp.float32).astype(jnp.bfloat16)
        inverse = lax.dot_general(
            items, hot, (((1,), (1,)), ((), ())), preferred_element_type=jnp.float32
        ).astype(jnp.int32)
        data_ref[c] = jnp.take_along_axis(data_ref[c], inverse, axis=1, mode="promise_in_bounds")

    for c in range(chunks):
        sort_chunk(c)
    copy.wait()
    sub8 = iota((8, LANES), 0)
    lane8 = iota((8, LANES), 1)

    def place_chunk(c, carry):
        row = data_ref[c]

        def place(o):
            off = meta_s[c, o]
            where_to = pl.ds(4 * (off >> 7), 8)
            turned = pltpu.roll(row, meta_s[c, devices + o], 1)
            keep = (sub8 < 4) & (lane8 < (off & (LANES - 1)))
            out_ref[o, where_to, :] = jnp.where(keep, out_ref[o, where_to, :], turned)

        each(devices, place, 8)
        return carry

    lax.fori_loop(0, chunks, place_chunk, 0, unroll=4 if devices <= 8 else 1)
    field_load.wait()


def greet(peers):
    barrier = pltpu.get_barrier_semaphore()
    for peer in peers:
        pl.semaphore_signal(barrier, inc=1, device_id=peer, device_id_type=MESH)
    return lambda: pl.semaphore_wait(barrier, len(peers))


def peer_along(axis, size, step):
    return {axis: lax.rem(lax.axis_index(axis) + step, size)}


def batch_of(tiles):
    return max(n for n in (4, 2, 1) if (tiles // 2) % n == 0)


def fused_kernel(
    devices, reps, tiles, out_in, field_ref, own_ref, rank_ref, meta_ref, cost_ref, grad_ref,
    meta_s, table, incoming, answers, landed, landed_last, index_v, index_s, cells, held, costs,
    meta_sem, index_sem, query_send, query_recv, answer_send, answer_recv, cost_send, cost_recv,
):
    lines = 4 * tiles
    pairs = tiles // 2
    total = devices * pairs
    batch = batch_of(tiles)
    batches = pairs // batch
    rooms = 2 if batch % 2 == 0 else 1
    bricks = field_ref.shape[0]
    me = lax.axis_index("map")
    meta_copy = pltpu.make_async_copy(meta_ref, meta_s, meta_sem)
    meta_copy.start()
    wait_peers = greet(
        [peer_along("map", devices, k) for k in range(1, devices)]
        + [peer_along("rep", reps, k) for k in range(1, reps)]
    )

    head = pairs // 2 // batch * batch

    def hop(j):
        if isinstance(j, int):
            return 2 if j == devices - 1 else j + (j >= 2)
        return jnp.where(j == devices - 1, 2, j + (j >= 2).astype(jnp.int32))

    if devices & (devices - 1) == 0:

        def asked(j):
            return lax.bitwise_xor(me, jnp.int32(hop(j)))

        asker = asked
    else:

        def asked(j):
            return lax.rem(me + j, devices)

        def asker(j):
            return lax.rem(me + devices - j, devices)

    def slot_rows(j):
        return pl.ds(pl.multiple_of(8 * (head + (j - 1) * pairs), 8), lines)

    def query_copy(j):
        return pltpu.make_async_remote_copy(
            src_ref=out_in.at[asked(j), pl.ds(0, lines)],
            dst_ref=incoming.at[slot_rows(j)],
            send_sem=query_send.at[j],
            recv_sem=query_recv.at[j],
            device_id={"map": asked(j)},
            device_id_type=MESH,
        )

    def answer_copy(j, last=False):
        return pltpu.make_async_remote_copy(
            src_ref=answers.at[slot_rows(j)],
            dst_ref=(landed_last if last else landed.at[j]).at[pl.ds(0, lines)],
            send_sem=answer_send.at[j],
            recv_sem=answer_recv.at[j],
            device_id={"map": asker(j)},
            device_id_type=MESH,
        )

    tail_row = 8 * (total - pairs + head)
    if head:
        incoming[0 : 8 * head] = out_in[me, 0 : 8 * head]
    incoming[tail_row:] = out_in[me, 8 * head : lines]
    cells[...] = jnp.zeros_like(cells)

    def build(g, carry):
        block = field_ref[pl.ds(pl.multiple_of(g * 16, 16), 16), :].astype(jnp.float32)
        for x in range(7):
            table[pl.ds(pl.multiple_of(x * bricks + g * 16, 16), 16), :] = block[:, 64 * x : 64 * x + 128]
        return carry

    wait_peers()
    each(devices - 1, lambda k: query_copy(k + 1).start(), 8)
    lax.fori_loop(0, bricks // 16, build, 0, unroll=32)

    def index_copy(slot):
        return pltpu.make_async_copy(index_v.at[slot], index_s.at[slot], index_sem.at[slot])

    def start_index(j, slot):
        first = pl.multiple_of(j * (8 * batch), 8)
        codes = incoming[pl.ds(first, 2 * batch, stride=4), :].astype(jnp.int32)
        row = ((codes >> 6) & 7) * bricks + (codes >> 9)
        index_v[slot] = jnp.clip(row, 0, 7 * bricks - 1)
        index_copy(slot).start()

    sub8 = iota((8, LANES), 0)

    def gather(slot, pair):
        for half in range(2):
            picked = [table[pl.ds(index_s[slot, 2 * pair + half, p], 1), :] for p in range(LANES)]
            cells[pair % rooms, half] = jnp.concatenate(picked, axis=0).T

    def weigh(g, now):
        query = incoming[pl.ds(pl.multiple_of(8 * g, 8), 8), :]
        code = query.astype(jnp.int32)
        results = []
        for half in range(2):
            row = 4 * half
            cy = jnp.broadcast_to((code[row : row + 1] >> 3) & 7, (8, LANES))
            cz = jnp.broadcast_to(code[row : row + 1] & 7, (8, LANES))
            fx = jnp.broadcast_to(query[row + 1 : row + 2], (8, LANES))
            fy = jnp.broadcast_to(query[row + 2 : row + 3], (8, LANES))
            fz = jnp.broadcast_to(query[row + 3 : row + 4], (8, LANES))
            is_y = [cy == y for y in range(7)]
            inter, slope = [], []
            for a in range(2):
                v = [cells[now, half, 64 * a + 8 * y : 64 * a + 8 * y + 8, :] for y in range(8)]
                low, high = v[0], v[1]
                for y in range(1, 7):
                    low = jnp.where(is_y[y], v[y], low)
                    high = jnp.where(is_y[y], v[y + 1], high)
                inter.append((1.0 - fy) * low + fy * high)
                slope.append(high - low)
            low, high = cz == sub8, cz == sub8 - 1
            weight = jnp.where(low, 1.0 - fz, jnp.where(high, fz, 0.0))
            sign = jnp.where(low, -1.0, jnp.where(high, 1.0, 0.0))
            mixed = (1.0 - fx) * inter[0] + fx * inter[1]
            results += [
                weight * mixed,
                weight * (inter[1] - inter[0]),
                weight * ((1.0 - fx) * slope[0] + fx * slope[1]),
                sign * mixed,
            ]
        for step in (4, 2, 1):
            upper = (sub8 & step) == 0
            count = len(results) // 2
            results = [
                jnp.where(upper, results[i], pltpu.roll(results[i + count], step, 0))
                + jnp.where(upper, pltpu.roll(results[i], 8 - step, 0), results[i + count])
                for i in range(count)
            ]
        answers[pl.ds(pl.multiple_of(8 * g, 8), 8), :] = results[0]

    def step(g, slot, pair):
        weigh(jnp.maximum(g - 1, 0), (pair + 1) % rooms)
        if slot is not None:
            gather(slot, pair)

    head_batches = head // batch
    count = devices * batches
    remote_end = head_batches + (devices - 1) * batches

    def finished(j):
        return ((j + 1) * batch - 1 - head + pairs) // pairs - 1

    def prepare(i, slot):
        following = 2 * i + slot + 1
        if batches == 2:
            fresh, origin = (slot == 0, i + 1)
        elif batches == 1:
            fresh, origin = (True, following + 1)
        else:
            past = following - head_batches + batches
            origin = past // batches
            fresh = (past % batches == 0) & (past >= batches)
        if fresh is not False:

            @pl.when((origin < devices) & fresh)
            def _():
                query_copy(origin).wait_recv()

        @pl.when(following < count)
        def _():
            start_index(following, 1 - slot)

    def segment(i, slot):
        j = 2 * i + slot
        if head_batches:
            late = j + 1 == head_batches
            pl.when(jnp.logical_not(late))(lambda: prepare(i, slot))
        else:
            prepare(i, slot)
        index_copy(slot).wait()
        for p in range(batch):
            step(j * batch + p, slot, p)
        if head_batches:
            pl.when(late)(lambda: prepare(i, slot))
        if batches == 2:
            done, ready = i, slot == 1
        elif batches == 1:
            done, ready = j, True
        else:
            done = finished(j)
            ready = done > finished(j - 1)
        if ready is not False:

            @pl.when(ready & (done > 0) & (done < devices - 1))
            def _():
                answer_copy(done).start()

    def double(i, carry):
        segment(i, 0)
        segment(i, 1)
        return carry

    if head_batches == 0:
        query_copy(1).wait_recv()
    start_index(0, 0)
    lax.fori_loop(0, count // 2, double, 0)
    early = min(max(finished(count - 1), 0), devices - 2)
    sent_last = finished(count - 1) >= devices - 1
    if sent_last:
        answer_copy(devices - 1, True).start()
    step(total, None, 0)
    if not sent_last:
        for k in range(early + 1, devices):
            answer_copy(k, k == devices - 1).start()
    if head:
        landed[0, 0 : 8 * head] = answers[0 : 8 * head]
    landed[0, 8 * head : lines] = answers[tail_row:]

    chunks = own_ref.shape[0]
    half = (sub8 >= 4).astype(jnp.int32)

    def collect(slots, first):
        def chunk(c, carry):
            owner = jnp.broadcast_to(own_ref[pl.ds(c, 1), :], (8, LANES))
            rank = jnp.broadcast_to(rank_ref[pl.ds(c, 1), :], (8, LANES))
            lane = rank & (LANES - 1)
            which = (rank >> 7) - half
            value = jnp.zeros((8, LANES), jnp.float32) if first else held[c]
            for k in slots:
                owner_k = asked(k) if k else me
                w = meta_s[c, owner_k] >> 7
                where = pl.ds(4 * w, 8)
                picked = jnp.take_along_axis(
                    landed_last[where, :] if k == devices - 1 else landed[k, where, :], lane, axis=1, mode="promise_in_bounds"
                )
                value = jnp.where((owner == owner_k) & (which == w), picked, value)
            held[c] = value
            return carry

        lax.fori_loop(0, chunks, chunk, 0, unroll=4 if devices <= 8 else 1)

    meta_copy.wait()
    each(devices - 2, lambda k: answer_copy(k + 1).wait_recv(), 8)
    collect(range(devices - 1), True)
    answer_copy(devices - 1, True).wait_recv()
    collect([devices - 1], False)
    dist = held[:, 0, :] + held[:, 4, :]
    hinge = jnp.maximum(margin - dist, 0.0)
    halves = grad_ref.shape[2] // LANES
    quarter = chunks // halves
    for h in range(halves):
        here = hinge[h * quarter : (h + 1) * quarter]
        costs[0, :, h * LANES : (h + 1) * LANES] = jnp.sum(here * here, axis=0, keepdims=True)
    sums = []
    for k in range(1, reps):
        copy = pltpu.make_async_remote_copy(
            src_ref=costs.at[0],
            dst_ref=costs.at[k],
            send_sem=cost_send.at[k],
            recv_sem=cost_recv.at[k],
            device_id=peer_along("rep", reps, k),
            device_id_type=MESH,
        )
        copy.start()
        sums.append(copy)
    for n in range(3):
        grad = -2.0 * hinge * (held[:, 1 + n, :] + held[:, 5 + n, :])
        for h in range(halves):
            grad_ref[n, :, h * LANES : (h + 1) * LANES] = grad[h * quarter : (h + 1) * quarter]

    each(devices - 1, lambda k: query_copy(k + 1).wait_send(), 8)
    each(devices - 2, lambda k: answer_copy(k + 1).wait_send(), 8)
    answer_copy(devices - 1, True).wait_send()
    total_cost = costs[0]
    for k, copy in enumerate(sums):
        copy.wait()
        total_cost = total_cost + costs[k + 1]
    cost_ref[...] = total_cost


def finish_kernel(cost_in, grad_in, cost_out, grad_out, sem):
    copies = [
        pltpu.make_async_copy(grad_in, grad_out, sem.at[0]),
        pltpu.make_async_copy(cost_in, cost_out, sem.at[1]),
    ]
    for copy in copies:
        copy.start()
    for copy in copies:
        copy.wait()


def per_device(field_bricks, owners, bricks, corners, fraction):
    devices = lax.axis_size("map")
    trajectories_here, quarter = owners.shape
    row_count = trajectories_here * quarter
    capacity = 4 * row_count // devices
    tiles = 2 * -(-capacity // (2 * LANES))
    chunks = row_count // LANES
    lines = 4 * tiles
    buffer = jax.ShapeDtypeStruct((devices, lines + 8, LANES), jnp.float32)
    flat = jax.ShapeDtypeStruct((chunks, LANES), jnp.int32)
    vm = pl.BlockSpec(memory_space=VMEM)
    sm = pl.BlockSpec(memory_space=SMEM)
    hbm = pl.BlockSpec(memory_space=pltpu.HBM)
    whole = VMEM((quarter, trajectories_here), jnp.int32)
    outgoing, own, rank, meta, field = pl.pallas_call(
        functools.partial(dispatch_kernel, devices, tiles),
        out_shape=(buffer, flat, flat, flat, jax.ShapeDtypeStruct(field_bricks.shape, field_bricks.dtype)),
        in_specs=[hbm] * 5,
        out_specs=(vm,) * 5,
        scratch_shapes=[
            VMEM((chunks, 8, LANES), jnp.float32),
            VMEM((chunks, LANES), jnp.int32),
            SMEM((chunks, LANES), jnp.int32),
            pltpu.SemaphoreType.DMA(()),
            whole, whole, whole,
            VMEM((3, quarter, trajectories_here), jnp.float32),
            pltpu.SemaphoreType.DMA((5,)),
        ],
        compiler_params=pltpu.CompilerParams(vmem_limit_bytes=16 << 20),
        name="dispatch",
    )(*(stay(x) for x in (owners.T, bricks.T, corners.T, fraction.transpose(0, 2, 1), field_bricks)))
    sems = pltpu.SemaphoreType.DMA((devices,))
    reps = lax.axis_size("rep")
    rep_sems = pltpu.SemaphoreType.DMA((reps,))
    batch = batch_of(tiles)
    square = VMEM((2 if batch % 2 == 0 else 1, 2, LANES, LANES), jnp.float32)
    bricks = field_bricks.shape[0]
    cost, waypoint_grad = pl.pallas_call(
        functools.partial(fused_kernel, devices, reps, tiles),
        out_shape=(
            jax.ShapeDtypeStruct((1, trajectories_here), jnp.float32),
            jax.ShapeDtypeStruct((3, quarter, trajectories_here), jnp.float32),
        ),
        in_specs=[vm] * 5,
        out_specs=(vm, vm),
        scratch_shapes=[
            SMEM((chunks, LANES), jnp.int32),
            VMEM((bricks * 7, LANES), jnp.float32),
            VMEM((devices * lines, LANES), jnp.float32),
            VMEM((devices * lines, LANES), jnp.float32),
            VMEM((devices - 1, lines + 8, LANES), jnp.float32),
            VMEM((lines + 8, LANES), jnp.float32),
            VMEM((2, 2 * batch, LANES), jnp.int32),
            SMEM((2, 2 * batch, LANES), jnp.int32),
            square,
            VMEM((chunks, 8, LANES), jnp.float32),
            VMEM((reps, 1, trajectories_here), jnp.float32),
            pltpu.SemaphoreType.DMA(()),
            pltpu.SemaphoreType.DMA((2,)),
            sems, sems, sems, sems, rep_sems, rep_sems,
        ],
        compiler_params=pltpu.CompilerParams(collective_id=0, has_side_effects=True, vmem_limit_bytes=24 << 20),
        name="fused",
    )(outgoing, field, own, rank, meta)
    cost, waypoint_grad = pl.pallas_call(
        finish_kernel,
        out_shape=(
            jax.ShapeDtypeStruct(cost.shape, jnp.float32),
            jax.ShapeDtypeStruct(waypoint_grad.shape, jnp.float32),
        ),
        in_specs=[vm] * 2,
        out_specs=(hbm,) * 2,
        scratch_shapes=[pltpu.SemaphoreType.DMA((2,))],
        compiler_params=pltpu.CompilerParams(vmem_limit_bytes=1 << 20),
        name="finish",
    )(cost, waypoint_grad)
    return cost.reshape(trajectories_here), waypoint_grad.transpose(0, 2, 1)


def solution(mesh):
    placed = (
        P("map", None),
        P("map", "rep"),
        P("map", "rep"),
        P("map", "rep"),
        P(None, "map", "rep"),
    )
    return jax.shard_map(
        per_device,
        mesh=mesh,
        in_specs=placed,
        out_specs=(P("map"), P(None, "map", "rep")),
        check_vma=False,
    )
```

```python
import functools

import jax
import jax.numpy as jnp
from jax import lax
from jax.experimental import pallas as pl
from jax.experimental.pallas import tpu as pltpu
from jax.sharding import PartitionSpec as P

margin = 0.5
LANES = 128
VMEM = pltpu.VMEM
SMEM = pltpu.SMEM


MESH = pl.DeviceIdType.MESH


def lanes_of(x):
    return jnp.concatenate(
        [x[:, h * LANES : (h + 1) * LANES] for h in range(x.shape[1] // LANES)], axis=0
    )


def iota(shape, axis):
    return lax.broadcasted_iota(jnp.int32, shape, axis)


def stay(x):
    return pltpu.with_memory_space_constraint(x, pltpu.HBM)


def each(count, body, unrolled):
    if count <= unrolled:
        for i in range(count):
            body(i)
    else:
        lax.fori_loop(0, count, lambda i, z: (body(i), z)[1], 0)


def dispatch_kernel(
    devices, tiles, owners_hbm, bricks_hbm, corners_hbm, frac_hbm, field_hbm,
    out_ref, own_ref, rank_ref, meta_ref, field_ref,
    data_ref, pos_ref, meta_s, sem, owners_ref, bricks_ref, corners_ref, frac_ref, load_sem, *piles,
):
    loads = [
        pltpu.make_async_copy(source, target, load_sem.at[i])
        for i, (source, target) in enumerate(
            [(owners_hbm, owners_ref), (bricks_hbm, bricks_ref),
             (corners_hbm, corners_ref), (frac_hbm, frac_ref)]
        )
    ]
    for load in loads:
        load.start()
    field_load = pltpu.make_async_copy(field_hbm, field_ref, load_sem.at[4])
    field_load.start()
    for pile in piles or (out_ref,):
        pile[...] = jnp.zeros_like(pile)
    for load in loads:
        load.wait()
    own = lanes_of(owners_ref[...])
    chunks = own.shape[0]
    bricks = bricks_ref[...]
    corners = corners_ref[...]
    cx = (corners * 1338) >> 16
    cxy = (corners * 9363) >> 16
    code = bricks * 512 + cx * 64 + (cxy - cx * 7) * 8 + (corners - cxy * 7)
    code = lanes_of(code.astype(jnp.float32))
    for k in range(2):
        data_ref[:, 4 * k, :] = code
    for f in range(3):
        part = lanes_of(frac_ref[f])
        for k in range(2):
            data_ref[:, 4 * k + 1 + f, :] = part
    own_ref[...] = own

    upper = (iota((LANES, LANES), 0) <= iota((LANES, LANES), 1)).astype(jnp.float32).astype(jnp.bfloat16)
    ones = jnp.ones((LANES, LANES), jnp.bfloat16)
    before = (iota((chunks, chunks), 0) > iota((chunks, chunks), 1)).astype(jnp.float32).astype(jnp.bfloat16)
    lane = iota((chunks, LANES), 1)
    rank = jnp.zeros((chunks, LANES), jnp.float32)
    pos = jnp.zeros((chunks, LANES), jnp.float32)
    start = jnp.zeros((chunks, LANES), jnp.float32)
    meta = jnp.zeros((chunks, LANES), jnp.int32)
    for o in range(devices):
        member = own == o
        m16 = member.astype(jnp.float32).astype(jnp.bfloat16)
        incl = jnp.dot(m16, upper, preferred_element_type=jnp.float32) - 1.0
        total = jnp.dot(m16, ones, preferred_element_type=jnp.float32)
        off = jnp.dot(before, total.astype(jnp.bfloat16), preferred_element_type=jnp.float32)
        rank = jnp.where(member, incl + off, rank)
        pos = jnp.where(member, incl + start, pos)
        meta = jnp.where(lane == o, off.astype(jnp.int32), meta)
        turn = (off - start).astype(jnp.int32) & (LANES - 1)
        meta = jnp.where(lane == devices + o, turn, meta)
        if piles:
            whole = off.astype(jnp.int32)
            meta = jnp.where(lane == 2 * devices + o, 4 * (whole >> 7), meta)
            meta = jnp.where(lane == 3 * devices + o, whole & (LANES - 1), meta)
        start = start + total
    rank_ref[...] = rank.astype(jnp.int32)
    pos_ref[...] = pos.astype(jnp.int32)
    meta_ref[...] = meta
    copy = pltpu.make_async_copy(meta_ref, meta_s, sem)
    copy.start()

    def sort_chunk(c):
        hot = (iota((LANES, LANES), 0) == pos_ref[pl.ds(c, 1), :]).astype(jnp.float32).astype(jnp.bfloat16)
        items = iota((8, LANES), 1).astype(jnp.float32).astype(jnp.bfloat16)
        inverse = lax.dot_general(
            items, hot, (((1,), (1,)), ((), ())), preferred_element_type=jnp.float32
        ).astype(jnp.int32)
        data_ref[c] = jnp.take_along_axis(data_ref[c], inverse, axis=1, mode="promise_in_bounds")

    for c in range(chunks):
        sort_chunk(c)
    copy.wait()
    sub8 = iota((8, LANES), 0)
    lane8 = iota((8, LANES), 1)

    def place_chunk(c, carry):
        row = data_ref[c]

        def place(o):
            off = meta_s[c, o]
            where_to = pl.ds(4 * (off >> 7), 8)
            turned = pltpu.roll(row, meta_s[c, devices + o], 1)
            keep = (sub8 < 4) & (lane8 < (off & (LANES - 1)))
            out_ref[o, where_to, :] = jnp.where(keep, out_ref[o, where_to, :], turned)

        if piles:
            for o, pile in enumerate(piles):
                where_to = pl.ds(meta_s[c, 2 * devices + o], 8)
                turned = pltpu.roll(row, meta_s[c, devices + o], 1)
                keep = (sub8 < 4) & (lane8 < meta_s[c, 3 * devices + o])
                pile[where_to, :] = jnp.where(keep, pile[where_to, :], turned)
        else:
            each(devices, place, 8)
        return carry

    lax.fori_loop(0, chunks, place_chunk, 0, unroll=8 if piles else 1)
    for o, pile in enumerate(piles):
        out_ref[o] = pile[...]
    field_load.wait()


def greet(peers):
    barrier = pltpu.get_barrier_semaphore()
    for peer in peers:
        pl.semaphore_signal(barrier, inc=1, device_id=peer, device_id_type=MESH)
    return lambda: pl.semaphore_wait(barrier, len(peers))


def peer_along(axis, size, step):
    return {axis: lax.rem(lax.axis_index(axis) + step, size)}


def batch_of(tiles):
    return max(n for n in (4, 2, 1) if (tiles // 2) % n == 0)


def fused_kernel(
    devices, reps, tiles, out_in, field_ref, own_ref, rank_ref, meta_ref, cost_ref, grad_ref,
    meta_s, table, incoming, answers, landed, landed_late, index_v, index_s, cells, held, costs,
    meta_sem, index_sem, query_send, query_recv, answer_send, answer_recv, cost_send, cost_recv,
):
    lines = 4 * tiles
    pairs = tiles // 2
    total = devices * pairs
    batch = batch_of(tiles)
    batches = pairs // batch
    rooms = 2 if batch % 2 == 0 else 1
    bricks = field_ref.shape[0]
    me = lax.axis_index("map")
    meta_copy = pltpu.make_async_copy(meta_ref, meta_s, meta_sem)
    meta_copy.start()
    wait_peers = greet(
        [peer_along("map", devices, k) for k in range(1, devices)]
        + [peer_along("rep", reps, k) for k in range(1, reps)]
    )

    head = pairs // 2 // batch * batch

    def hop(j):
        if isinstance(j, int):
            return 2 if j == devices - 1 else j + (j >= 2)
        return jnp.where(j == devices - 1, 2, j + (j >= 2).astype(jnp.int32))

    if devices & (devices - 1) == 0:

        def asked(j):
            return lax.bitwise_xor(me, jnp.int32(hop(j)))

        asker = asked
    else:

        def asked(j):
            return lax.rem(me + j, devices)

        def asker(j):
            return lax.rem(me + devices - j, devices)

    def slot_rows(j):
        return pl.ds(pl.multiple_of(8 * (head + (j - 1) * pairs), 8), lines)

    def query_copy(j):
        return pltpu.make_async_remote_copy(
            src_ref=out_in.at[asked(j), pl.ds(0, lines)],
            dst_ref=incoming.at[slot_rows(j)],
            send_sem=query_send.at[j],
            recv_sem=query_recv.at[j],
            device_id={"map": asked(j)},
            device_id_type=MESH,
        )

    keep = devices - 2

    def answer_copy(j, late=False):
        return pltpu.make_async_remote_copy(
            src_ref=answers.at[slot_rows(j)],
            dst_ref=(landed_late.at[j - keep] if late else landed.at[j]).at[pl.ds(0, lines)],
            send_sem=answer_send.at[j],
            recv_sem=answer_recv.at[j],
            device_id={"map": asker(j)},
            device_id_type=MESH,
        )

    tail_row = 8 * (total - pairs + head)
    if head:
        incoming[0 : 8 * head] = out_in[me, 0 : 8 * head]
    incoming[tail_row:] = out_in[me, 8 * head : lines]
    cells[...] = jnp.zeros_like(cells)

    def build(g, carry):
        block = field_ref[pl.ds(pl.multiple_of(g * 16, 16), 16), :].astype(jnp.float32)
        for x in range(7):
            table[pl.ds(pl.multiple_of(x * bricks + g * 16, 16), 16), :] = block[:, 64 * x : 64 * x + 128]
        return carry

    wait_peers()
    each(devices - 1, lambda k: query_copy(k + 1).start(), 8)
    lax.fori_loop(0, bricks // 16, build, 0, unroll=32)

    def index_copy(slot):
        return pltpu.make_async_copy(index_v.at[slot], index_s.at[slot], index_sem.at[slot])

    def start_index(j, slot):
        first = pl.multiple_of(j * (8 * batch), 8)
        codes = incoming[pl.ds(first, 2 * batch, stride=4), :].astype(jnp.int32)
        row = ((codes >> 6) & 7) * bricks + (codes >> 9)
        index_v[slot] = jnp.clip(row, 0, 7 * bricks - 1)
        index_copy(slot).start()

    sub8 = iota((8, LANES), 0)

    def gather(slot, pair):
        for half in range(2):
            picked = [table[pl.ds(index_s[slot, 2 * pair + half, p], 1), :] for p in range(LANES)]
            cells[pair % rooms, half] = jnp.concatenate(picked, axis=0).T

    def weigh(g, now):
        query = incoming[pl.ds(pl.multiple_of(8 * g, 8), 8), :]
        code = query.astype(jnp.int32)
        results = []
        for half in range(2):
            row = 4 * half
            cy = jnp.broadcast_to((code[row : row + 1] >> 3) & 7, (8, LANES))
            cz = jnp.broadcast_to(code[row : row + 1] & 7, (8, LANES))
            fx = jnp.broadcast_to(query[row + 1 : row + 2], (8, LANES))
            fy = jnp.broadcast_to(query[row + 2 : row + 3], (8, LANES))
            fz = jnp.broadcast_to(query[row + 3 : row + 4], (8, LANES))
            is_y = [cy == y for y in range(7)]
            inter, slope = [], []
            for a in range(2):
                v = [cells[now, half, 64 * a + 8 * y : 64 * a + 8 * y + 8, :] for y in range(8)]
                low, high = v[0], v[1]
                for y in range(1, 7):
                    low = jnp.where(is_y[y], v[y], low)
                    high = jnp.where(is_y[y], v[y + 1], high)
                inter.append((1.0 - fy) * low + fy * high)
                slope.append(high - low)
            low, high = cz == sub8, cz == sub8 - 1
            weight = jnp.where(low, 1.0 - fz, jnp.where(high, fz, 0.0))
            sign = jnp.where(low, -1.0, jnp.where(high, 1.0, 0.0))
            mixed = (1.0 - fx) * inter[0] + fx * inter[1]
            results += [
                weight * mixed,
                weight * (inter[1] - inter[0]),
                weight * ((1.0 - fx) * slope[0] + fx * slope[1]),
                sign * mixed,
            ]
        for step in (4, 2, 1):
            upper = (sub8 & step) == 0
            count = len(results) // 2
            results = [
                jnp.where(upper, results[i], pltpu.roll(results[i + count], step, 0))
                + jnp.where(upper, pltpu.roll(results[i], 8 - step, 0), results[i + count])
                for i in range(count)
            ]
        answers[pl.ds(pl.multiple_of(8 * g, 8), 8), :] = results[0]

    def step(g, slot, pair):
        weigh(jnp.maximum(g - 1, 0), (pair + 1) % rooms)
        if slot is not None:
            gather(slot, pair)

    head_batches = head // batch
    count = devices * batches
    remote_end = head_batches + (devices - 1) * batches

    def finished(j):
        return ((j + 1) * batch - 1 - head + pairs) // pairs - 1

    def prepare(i, slot):
        following = 2 * i + slot + 1
        if batches == 2:
            fresh, origin = (slot == 0, i + 1)
        elif batches == 1:
            fresh, origin = (True, following + 1)
        else:
            past = following - head_batches + batches
            origin = past // batches
            fresh = (past % batches == 0) & (past >= batches)
        if fresh is not False:

            @pl.when((origin < devices) & fresh)
            def _():
                query_copy(origin).wait_recv()

        @pl.when(following < count)
        def _():
            start_index(following, 1 - slot)

    def segment(i, slot, final=False):
        j = 2 * i + slot
        if head_batches:
            late = j + 1 == head_batches
            pl.when(jnp.logical_not(late))(lambda: prepare(i, slot))
        else:
            prepare(i, slot)
        index_copy(slot).wait()
        for p in range(batch):
            step(j * batch + p, slot, p)
            if final and p == min(1, batch - 1):
                answer_copy(devices - 1, True).start()
        if head_batches:
            pl.when(late)(lambda: prepare(i, slot))
        if batches == 2:
            done, ready = i, slot == 1
        elif batches == 1:
            done, ready = j, True
        else:
            done = finished(j)
            ready = done > finished(j - 1)
        if ready is not False and not final:

            @pl.when(ready & (done > 0) & (done < keep))
            def _():
                answer_copy(done).start()

            @pl.when(ready & (done == keep))
            def _():
                answer_copy(keep, True).start()

    def double(i, carry):
        segment(i, 0)
        segment(i, 1)
        return carry

    if head_batches == 0:
        query_copy(1).wait_recv()
    start_index(0, 0)
    lax.fori_loop(0, count // 2 - 1, double, 0)
    segment(jnp.int32(count // 2 - 1), 0)
    segment(jnp.int32(count // 2 - 1), 1, True)
    step(total, None, 0)
    if head:
        landed[0, 0 : 8 * head] = answers[0 : 8 * head]
    landed[0, 8 * head : lines] = answers[tail_row:]

    chunks = own_ref.shape[0]
    half = (sub8 >= 4).astype(jnp.int32)

    def collect(slots, first, unroll):
        def chunk(c, carry):
            owner = jnp.broadcast_to(own_ref[pl.ds(c, 1), :], (8, LANES))
            rank = jnp.broadcast_to(rank_ref[pl.ds(c, 1), :], (8, LANES))
            lane = rank & (LANES - 1)
            which = (rank >> 7) - half
            value = jnp.zeros((8, LANES), jnp.float32) if first else held[c]
            for k in slots:
                owner_k = asked(k) if k else me
                w = meta_s[c, owner_k] >> 7
                where = pl.ds(4 * w, 8)
                picked = jnp.take_along_axis(
                    landed_late[k - keep, where, :] if k >= keep else landed[k, where, :], lane, axis=1, mode="promise_in_bounds"
                )
                value = jnp.where((owner == owner_k) & (which == w), picked, value)
            held[c] = value
            return carry

        lax.fori_loop(0, chunks, chunk, 0, unroll=unroll if devices <= 8 else 1)

    meta_copy.wait()
    each(keep - 1, lambda k: answer_copy(k + 1).wait_recv(), 8)
    collect(range(keep), True, 8)
    for k in (keep, keep + 1):
        answer_copy(k, True).wait_recv()
    collect((keep, keep + 1), False, 16)
    dist = held[:, 0, :] + held[:, 4, :]
    hinge = jnp.maximum(margin - dist, 0.0)
    halves = grad_ref.shape[2] // LANES
    quarter = chunks // halves
    for h in range(halves):
        here = hinge[h * quarter : (h + 1) * quarter]
        costs[0, :, h * LANES : (h + 1) * LANES] = jnp.sum(here * here, axis=0, keepdims=True)
    sums = []
    for k in range(1, reps):
        copy = pltpu.make_async_remote_copy(
            src_ref=costs.at[0],
            dst_ref=costs.at[k],
            send_sem=cost_send.at[k],
            recv_sem=cost_recv.at[k],
            device_id=peer_along("rep", reps, k),
            device_id_type=MESH,
        )
        copy.start()
        sums.append(copy)
    for n in range(3):
        grad = -2.0 * hinge * (held[:, 1 + n, :] + held[:, 5 + n, :])
        for h in range(halves):
            grad_ref[n, :, h * LANES : (h + 1) * LANES] = grad[h * quarter : (h + 1) * quarter]

    each(devices - 1, lambda k: query_copy(k + 1).wait_send(), 8)
    each(keep - 1, lambda k: answer_copy(k + 1).wait_send(), 8)
    for k in (keep, keep + 1):
        answer_copy(k, True).wait_send()
    total_cost = costs[0]
    for k, copy in enumerate(sums):
        copy.wait()
        total_cost = total_cost + costs[k + 1]
    cost_ref[...] = total_cost


def finish_kernel(cost_in, grad_in, cost_out, grad_out, sem):
    copies = [
        pltpu.make_async_copy(grad_in, grad_out, sem.at[0]),
        pltpu.make_async_copy(cost_in, cost_out, sem.at[1]),
    ]
    for copy in copies:
        copy.start()
    for copy in copies:
        copy.wait()


def per_device(field_bricks, owners, bricks, corners, fraction):
    devices = lax.axis_size("map")
    trajectories_here, quarter = owners.shape
    row_count = trajectories_here * quarter
    capacity = 4 * row_count // devices
    tiles = 2 * -(-capacity // (2 * LANES))
    chunks = row_count // LANES
    lines = 4 * tiles
    buffer = jax.ShapeDtypeStruct((devices, lines + 8, LANES), jnp.float32)
    flat = jax.ShapeDtypeStruct((chunks, LANES), jnp.int32)
    vm = pl.BlockSpec(memory_space=VMEM)
    sm = pl.BlockSpec(memory_space=SMEM)
    hbm = pl.BlockSpec(memory_space=pltpu.HBM)
    whole = VMEM((quarter, trajectories_here), jnp.int32)
    outgoing, own, rank, meta, field = pl.pallas_call(
        functools.partial(dispatch_kernel, devices, tiles),
        out_shape=(buffer, flat, flat, flat, jax.ShapeDtypeStruct(field_bricks.shape, field_bricks.dtype)),
        in_specs=[hbm] * 5,
        out_specs=(vm,) * 5,
        scratch_shapes=[
            VMEM((chunks, 8, LANES), jnp.float32),
            VMEM((chunks, LANES), jnp.int32),
            SMEM((chunks, LANES), jnp.int32),
            pltpu.SemaphoreType.DMA(()),
            whole, whole, whole,
            VMEM((3, quarter, trajectories_here), jnp.float32),
            pltpu.SemaphoreType.DMA((5,)),
        ]
        + [VMEM((lines + 8, LANES), jnp.float32)] * (devices if devices <= 8 else 0),
        compiler_params=pltpu.CompilerParams(vmem_limit_bytes=16 << 20),
        name="dispatch",
    )(*(stay(x) for x in (owners.T, bricks.T, corners.T, fraction.transpose(0, 2, 1), field_bricks)))
    sems = pltpu.SemaphoreType.DMA((devices,))
    reps = lax.axis_size("rep")
    rep_sems = pltpu.SemaphoreType.DMA((reps,))
    batch = batch_of(tiles)
    square = VMEM((2 if batch % 2 == 0 else 1, 2, LANES, LANES), jnp.float32)
    bricks = field_bricks.shape[0]
    cost, waypoint_grad = pl.pallas_call(
        functools.partial(fused_kernel, devices, reps, tiles),
        out_shape=(
            jax.ShapeDtypeStruct((1, trajectories_here), jnp.float32),
            jax.ShapeDtypeStruct((3, quarter, trajectories_here), jnp.float32),
        ),
        in_specs=[vm] * 5,
        out_specs=(vm, vm),
        scratch_shapes=[
            SMEM((chunks, LANES), jnp.int32),
            VMEM((bricks * 7, LANES), jnp.float32),
            VMEM((devices * lines, LANES), jnp.float32),
            VMEM((devices * lines, LANES), jnp.float32),
            VMEM((devices - 2, lines + 8, LANES), jnp.float32),
            VMEM((2, lines + 8, LANES), jnp.float32),
            VMEM((2, 2 * batch, LANES), jnp.int32),
            SMEM((2, 2 * batch, LANES), jnp.int32),
            square,
            VMEM((chunks, 8, LANES), jnp.float32),
            VMEM((reps, 1, trajectories_here), jnp.float32),
            pltpu.SemaphoreType.DMA(()),
            pltpu.SemaphoreType.DMA((2,)),
            sems, sems, sems, sems, rep_sems, rep_sems,
        ],
        compiler_params=pltpu.CompilerParams(collective_id=0, has_side_effects=True, vmem_limit_bytes=24 << 20),
        name="fused",
    )(outgoing, field, own, rank, meta)
    cost, waypoint_grad = pl.pallas_call(
        finish_kernel,
        out_shape=(
            jax.ShapeDtypeStruct(cost.shape, jnp.float32),
            jax.ShapeDtypeStruct(waypoint_grad.shape, jnp.float32),
        ),
        in_specs=[vm] * 2,
        out_specs=(hbm,) * 2,
        scratch_shapes=[pltpu.SemaphoreType.DMA((2,))],
        compiler_params=pltpu.CompilerParams(vmem_limit_bytes=1 << 20),
        name="finish",
    )(cost, waypoint_grad)
    return cost.reshape(trajectories_here), waypoint_grad.transpose(0, 2, 1)


def solution(mesh):
    placed = (
        P("map", None),
        P("map", "rep"),
        P("map", "rep"),
        P("map", "rep"),
        P(None, "map", "rep"),
    )
    return jax.shard_map(
        per_device,
        mesh=mesh,
        in_specs=placed,
        out_specs=(P("map"), P(None, "map", "rep")),
        check_vma=False,
    )
```

```python
import functools

import jax
import jax.numpy as jnp
from jax import lax
from jax.experimental import pallas as pl
from jax.experimental.pallas import tpu as pltpu
from jax.sharding import PartitionSpec as P

margin = 0.5
LANES = 128
VMEM = pltpu.VMEM
SMEM = pltpu.SMEM


MESH = pl.DeviceIdType.MESH


def lanes_of(x):
    return jnp.concatenate(
        [x[:, h * LANES : (h + 1) * LANES] for h in range(x.shape[1] // LANES)], axis=0
    )


def iota(shape, axis):
    return lax.broadcasted_iota(jnp.int32, shape, axis)


def stay(x):
    return pltpu.with_memory_space_constraint(x, pltpu.HBM)


def each(count, body, unrolled):
    if count <= unrolled:
        for i in range(count):
            body(i)
    else:
        lax.fori_loop(0, count, lambda i, z: (body(i), z)[1], 0)


def dispatch_kernel(
    devices, tiles, owners_hbm, bricks_hbm, corners_hbm, frac_hbm, field_hbm,
    out_ref, own_ref, rank_ref, meta_ref, field_ref,
    data_ref, pos_ref, meta_s, sem, owners_ref, bricks_ref, corners_ref, frac_ref, load_sem, *piles,
):
    loads = [
        pltpu.make_async_copy(source, target, load_sem.at[i])
        for i, (source, target) in enumerate(
            [(owners_hbm, owners_ref), (bricks_hbm, bricks_ref),
             (corners_hbm, corners_ref), (frac_hbm, frac_ref)]
        )
    ]
    for load in loads:
        load.start()
    field_load = pltpu.make_async_copy(field_hbm, field_ref, load_sem.at[4])
    field_load.start()
    for pile in piles or (out_ref,):
        pile[...] = jnp.zeros_like(pile)
    for load in loads:
        load.wait()
    own = lanes_of(owners_ref[...])
    chunks = own.shape[0]
    bricks = bricks_ref[...]
    corners = corners_ref[...]
    cx = (corners * 1338) >> 16
    cxy = (corners * 9363) >> 16
    code = bricks * 512 + cx * 64 + (cxy - cx * 7) * 8 + (corners - cxy * 7)
    code = lanes_of(code.astype(jnp.float32))
    for k in range(2):
        data_ref[:, 4 * k, :] = code
    for f in range(3):
        part = lanes_of(frac_ref[f])
        for k in range(2):
            data_ref[:, 4 * k + 1 + f, :] = part
    own_ref[...] = own

    upper = (iota((LANES, LANES), 0) <= iota((LANES, LANES), 1)).astype(jnp.float32).astype(jnp.bfloat16)
    ones = jnp.ones((LANES, LANES), jnp.bfloat16)
    before = (iota((chunks, chunks), 0) > iota((chunks, chunks), 1)).astype(jnp.float32).astype(jnp.bfloat16)
    lane = iota((chunks, LANES), 1)
    rank = jnp.zeros((chunks, LANES), jnp.float32)
    pos = jnp.zeros((chunks, LANES), jnp.float32)
    start = jnp.zeros((chunks, LANES), jnp.float32)
    meta = jnp.zeros((chunks, LANES), jnp.int32)
    if piles:
        stacked = jnp.concatenate(
            [(own == o).astype(jnp.float32) for o in range(devices)], axis=0
        ).astype(jnp.bfloat16)
        both = jnp.dot(
            stacked, jnp.concatenate([upper, ones], axis=1), preferred_element_type=jnp.float32
        )
        totals = both[:, LANES:]
        size = devices * chunks
        down, across = iota((size, size), 0), iota((size, size), 1)
        same = (down // chunks == across // chunks) & (down > across)
        offs = jnp.dot(
            same.astype(jnp.float32).astype(jnp.bfloat16), totals.astype(jnp.bfloat16),
            preferred_element_type=jnp.float32,
        )
    for o in range(devices):
        member = own == o
        if piles:
            here = slice(o * chunks, (o + 1) * chunks)
            incl, total, off = both[here, :LANES] - 1.0, totals[here], offs[here]
        else:
            m16 = member.astype(jnp.float32).astype(jnp.bfloat16)
            incl = jnp.dot(m16, upper, preferred_element_type=jnp.float32) - 1.0
            total = jnp.dot(m16, ones, preferred_element_type=jnp.float32)
            off = jnp.dot(before, total.astype(jnp.bfloat16), preferred_element_type=jnp.float32)
        rank = jnp.where(member, incl + off, rank)
        pos = jnp.where(member, incl + start, pos)
        meta = jnp.where(lane == o, off.astype(jnp.int32), meta)
        turn = (off - start).astype(jnp.int32) & (LANES - 1)
        meta = jnp.where(lane == devices + o, turn, meta)
        if piles:
            whole = off.astype(jnp.int32)
            meta = jnp.where(lane == 2 * devices + o, 4 * (whole >> 7), meta)
            meta = jnp.where(lane == 3 * devices + o, whole & (LANES - 1), meta)
        start = start + total
    rank_ref[...] = rank.astype(jnp.int32)
    pos_ref[...] = pos.astype(jnp.int32)
    meta_ref[...] = meta
    copy = pltpu.make_async_copy(meta_ref, meta_s, sem)
    copy.start()

    def sort_chunk(c):
        hot = (iota((LANES, LANES), 0) == pos_ref[pl.ds(c, 1), :]).astype(jnp.float32).astype(jnp.bfloat16)
        items = iota((8, LANES), 1).astype(jnp.float32).astype(jnp.bfloat16)
        inverse = lax.dot_general(
            items, hot, (((1,), (1,)), ((), ())), preferred_element_type=jnp.float32
        ).astype(jnp.int32)
        data_ref[c] = jnp.take_along_axis(data_ref[c], inverse, axis=1, mode="promise_in_bounds")

    for c in range(chunks):
        sort_chunk(c)
    copy.wait()
    sub8 = iota((8, LANES), 0)
    lane8 = iota((8, LANES), 1)

    def place_chunk(c, carry):
        row = data_ref[c]

        def place(o):
            off = meta_s[c, o]
            where_to = pl.ds(4 * (off >> 7), 8)
            turned = pltpu.roll(row, meta_s[c, devices + o], 1)
            keep = (sub8 < 4) & (lane8 < (off & (LANES - 1)))
            out_ref[o, where_to, :] = jnp.where(keep, out_ref[o, where_to, :], turned)

        if piles:
            for o, pile in enumerate(piles):
                where_to = pl.ds(meta_s[c, 2 * devices + o], 8)
                turned = pltpu.roll(row, meta_s[c, devices + o], 1)
                keep = (sub8 < 4) & (lane8 < meta_s[c, 3 * devices + o])
                pile[where_to, :] = jnp.where(keep, pile[where_to, :], turned)
        else:
            each(devices, place, 8)
        return carry

    lax.fori_loop(0, chunks, place_chunk, 0, unroll=16 if piles else 1)
    for o, pile in enumerate(piles):
        out_ref[o] = pile[...]
    field_load.wait()


def greet(peers):
    barrier = pltpu.get_barrier_semaphore()
    for peer in peers:
        pl.semaphore_signal(barrier, inc=1, device_id=peer, device_id_type=MESH)
    return lambda: pl.semaphore_wait(barrier, len(peers))


def peer_along(axis, size, step):
    return {axis: lax.rem(lax.axis_index(axis) + step, size)}


def batch_of(tiles):
    return max(n for n in (4, 2, 1) if (tiles // 2) % n == 0)


def fused_kernel(
    devices, reps, tiles, out_in, field_ref, own_ref, rank_ref, meta_ref, cost_ref, grad_ref,
    meta_s, table, incoming, answers, landed, landed_late, index_v, index_s, cells, held, costs,
    meta_sem, index_sem, query_send, query_recv, answer_send, answer_recv, cost_send, cost_recv,
):
    lines = 4 * tiles
    pairs = tiles // 2
    total = devices * pairs
    batch = batch_of(tiles)
    batches = pairs // batch
    rooms = 2 if batch % 2 == 0 else 1
    bricks = field_ref.shape[0]
    me = lax.axis_index("map")
    meta_copy = pltpu.make_async_copy(meta_ref, meta_s, meta_sem)
    meta_copy.start()
    wait_peers = greet(
        [peer_along("map", devices, k) for k in range(1, devices)]
        + [peer_along("rep", reps, k) for k in range(1, reps)]
    )

    head = pairs // 2 // batch * batch

    def hop(j):
        if isinstance(j, int):
            return 2 if j == devices - 1 else j + (j >= 2)
        return jnp.where(j == devices - 1, 2, j + (j >= 2).astype(jnp.int32))

    if devices & (devices - 1) == 0:

        def asked(j):
            return lax.bitwise_xor(me, jnp.int32(hop(j)))

        asker = asked
    else:

        def asked(j):
            return lax.rem(me + j, devices)

        def asker(j):
            return lax.rem(me + devices - j, devices)

    def slot_rows(j):
        return pl.ds(pl.multiple_of(8 * (head + (j - 1) * pairs), 8), lines)

    def query_copy(j):
        return pltpu.make_async_remote_copy(
            src_ref=out_in.at[asked(j), pl.ds(0, lines)],
            dst_ref=incoming.at[slot_rows(j)],
            send_sem=query_send.at[j],
            recv_sem=query_recv.at[j],
            device_id={"map": asked(j)},
            device_id_type=MESH,
        )

    keep = devices - 2

    def answer_copy(j, late=False):
        return pltpu.make_async_remote_copy(
            src_ref=answers.at[slot_rows(j)],
            dst_ref=(landed_late.at[j - keep] if late else landed.at[j]).at[pl.ds(0, lines)],
            send_sem=answer_send.at[j],
            recv_sem=answer_recv.at[j],
            device_id={"map": asker(j)},
            device_id_type=MESH,
        )

    tail_row = 8 * (total - pairs + head)
    if head:
        incoming[0 : 8 * head] = out_in[me, 0 : 8 * head]
    incoming[tail_row:] = out_in[me, 8 * head : lines]
    cells[...] = jnp.zeros_like(cells)

    def build(g, carry):
        block = field_ref[pl.ds(pl.multiple_of(g * 16, 16), 16), :].astype(jnp.float32)
        for x in range(7):
            table[pl.ds(pl.multiple_of(x * bricks + g * 16, 16), 16), :] = block[:, 64 * x : 64 * x + 128]
        return carry

    wait_peers()
    each(devices - 1, lambda k: query_copy(k + 1).start(), 8)
    lax.fori_loop(0, bricks // 16, build, 0, unroll=64)

    def index_copy(slot):
        return pltpu.make_async_copy(index_v.at[slot], index_s.at[slot], index_sem.at[slot])

    def start_index(j, slot):
        first = pl.multiple_of(j * (8 * batch), 8)
        codes = incoming[pl.ds(first, 2 * batch, stride=4), :].astype(jnp.int32)
        row = ((codes >> 6) & 7) * bricks + (codes >> 9)
        index_v[slot] = jnp.clip(row, 0, 7 * bricks - 1)
        index_copy(slot).start()

    sub8 = iota((8, LANES), 0)

    def gather(slot, pair):
        for half in range(2):
            picked = [table[pl.ds(index_s[slot, 2 * pair + half, p], 1), :] for p in range(LANES)]
            cells[pair % rooms, half] = jnp.concatenate(picked, axis=0).T

    def weigh(g, now):
        query = incoming[pl.ds(pl.multiple_of(8 * g, 8), 8), :]
        code = query.astype(jnp.int32)
        results = []
        for half in range(2):
            row = 4 * half
            cy = jnp.broadcast_to((code[row : row + 1] >> 3) & 7, (8, LANES))
            cz = jnp.broadcast_to(code[row : row + 1] & 7, (8, LANES))
            fx = jnp.broadcast_to(query[row + 1 : row + 2], (8, LANES))
            fy = jnp.broadcast_to(query[row + 2 : row + 3], (8, LANES))
            fz = jnp.broadcast_to(query[row + 3 : row + 4], (8, LANES))
            is_y = [cy == y for y in range(7)]
            inter, slope = [], []
            for a in range(2):
                v = [cells[now, half, 64 * a + 8 * y : 64 * a + 8 * y + 8, :] for y in range(8)]
                low, high = v[0], v[1]
                for y in range(1, 7):
                    low = jnp.where(is_y[y], v[y], low)
                    high = jnp.where(is_y[y], v[y + 1], high)
                inter.append((1.0 - fy) * low + fy * high)
                slope.append(high - low)
            low, high = cz == sub8, cz == sub8 - 1
            weight = jnp.where(low, 1.0 - fz, jnp.where(high, fz, 0.0))
            sign = jnp.where(low, -1.0, jnp.where(high, 1.0, 0.0))
            mixed = (1.0 - fx) * inter[0] + fx * inter[1]
            results += [
                weight * mixed,
                weight * (inter[1] - inter[0]),
                weight * ((1.0 - fx) * slope[0] + fx * slope[1]),
                sign * mixed,
            ]
        for step in (4, 2, 1):
            upper = (sub8 & step) == 0
            count = len(results) // 2
            results = [
                jnp.where(upper, results[i], pltpu.roll(results[i + count], step, 0))
                + jnp.where(upper, pltpu.roll(results[i], 8 - step, 0), results[i + count])
                for i in range(count)
            ]
        answers[pl.ds(pl.multiple_of(8 * g, 8), 8), :] = results[0]

    def step(g, slot, pair):
        weigh(jnp.maximum(g - 1, 0), (pair + 1) % rooms)
        if slot is not None:
            gather(slot, pair)

    head_batches = head // batch
    count = devices * batches
    remote_end = head_batches + (devices - 1) * batches

    def finished(j):
        return ((j + 1) * batch - 1 - head + pairs) // pairs - 1

    def prepare(i, slot):
        following = 2 * i + slot + 1
        if batches == 2:
            fresh, origin = (slot == 0, i + 1)
        elif batches == 1:
            fresh, origin = (True, following + 1)
        else:
            past = following - head_batches + batches
            origin = past // batches
            fresh = (past % batches == 0) & (past >= batches)
        if fresh is not False:

            @pl.when((origin < devices) & fresh)
            def _():
                query_copy(origin).wait_recv()

        @pl.when(following < count)
        def _():
            start_index(following, 1 - slot)

    def segment(i, slot, final=False):
        j = 2 * i + slot
        if head_batches:
            late = j + 1 == head_batches
            pl.when(jnp.logical_not(late))(lambda: prepare(i, slot))
        else:
            prepare(i, slot)
        index_copy(slot).wait()
        for p in range(batch):
            step(j * batch + p, slot, p)
            if final and p == min(1, batch - 1):
                answer_copy(devices - 1, True).start()
        if head_batches:
            pl.when(late)(lambda: prepare(i, slot))
        if batches == 2:
            done, ready = i, slot == 1
        elif batches == 1:
            done, ready = j, True
        else:
            done = finished(j)
            ready = done > finished(j - 1)
        if ready is not False and not final:

            @pl.when(ready & (done > 0) & (done < keep))
            def _():
                answer_copy(done).start()

            @pl.when(ready & (done == keep))
            def _():
                answer_copy(keep, True).start()

    def double(i, carry):
        segment(i, 0)
        segment(i, 1)
        return carry

    if head_batches == 0:
        query_copy(1).wait_recv()
    start_index(0, 0)
    lax.fori_loop(0, count // 2 - 1, double, 0)
    segment(jnp.int32(count // 2 - 1), 0)
    segment(jnp.int32(count // 2 - 1), 1, True)
    step(total, None, 0)
    if head:
        landed[0, 0 : 8 * head] = answers[0 : 8 * head]
    landed[0, 8 * head : lines] = answers[tail_row:]

    chunks = own_ref.shape[0]
    half = (sub8 >= 4).astype(jnp.int32)

    def collect(slots, first, unroll):
        def chunk(c, carry):
            owner = jnp.broadcast_to(own_ref[pl.ds(c, 1), :], (8, LANES))
            rank = jnp.broadcast_to(rank_ref[pl.ds(c, 1), :], (8, LANES))
            lane = rank & (LANES - 1)
            which = (rank >> 7) - half
            value = jnp.zeros((8, LANES), jnp.float32) if first else held[c]
            for k in slots:
                owner_k = asked(k) if k else me
                w = meta_s[c, owner_k] >> 7
                where = pl.ds(4 * w, 8)
                picked = jnp.take_along_axis(
                    landed_late[k - keep, where, :] if k >= keep else landed[k, where, :], lane, axis=1, mode="promise_in_bounds"
                )
                value = jnp.where((owner == owner_k) & (which == w), picked, value)
            held[c] = value
            return carry

        lax.fori_loop(0, chunks, chunk, 0, unroll=unroll if devices <= 8 else 1)

    meta_copy.wait()
    each(keep - 1, lambda k: answer_copy(k + 1).wait_recv(), 8)
    collect(range(keep), True, 16)
    for k in (keep, keep + 1):
        answer_copy(k, True).wait_recv()
    collect((keep, keep + 1), False, 32)
    dist = held[:, 0, :] + held[:, 4, :]
    hinge = jnp.maximum(margin - dist, 0.0)
    halves = grad_ref.shape[2] // LANES
    quarter = chunks // halves
    for h in range(halves):
        here = hinge[h * quarter : (h + 1) * quarter]
        costs[0, :, h * LANES : (h + 1) * LANES] = jnp.sum(here * here, axis=0, keepdims=True)
    sums = []
    for k in range(1, reps):
        copy = pltpu.make_async_remote_copy(
            src_ref=costs.at[0],
            dst_ref=costs.at[k],
            send_sem=cost_send.at[k],
            recv_sem=cost_recv.at[k],
            device_id=peer_along("rep", reps, k),
            device_id_type=MESH,
        )
        copy.start()
        sums.append(copy)
    for n in range(3):
        grad = -2.0 * hinge * (held[:, 1 + n, :] + held[:, 5 + n, :])
        for h in range(halves):
            grad_ref[n, :, h * LANES : (h + 1) * LANES] = grad[h * quarter : (h + 1) * quarter]

    each(devices - 1, lambda k: query_copy(k + 1).wait_send(), 8)
    each(keep - 1, lambda k: answer_copy(k + 1).wait_send(), 8)
    for k in (keep, keep + 1):
        answer_copy(k, True).wait_send()
    total_cost = costs[0]
    for k, copy in enumerate(sums):
        copy.wait()
        total_cost = total_cost + costs[k + 1]
    cost_ref[...] = total_cost


def finish_kernel(cost_in, grad_in, cost_out, grad_out, sem):
    copies = [
        pltpu.make_async_copy(grad_in, grad_out, sem.at[0]),
        pltpu.make_async_copy(cost_in, cost_out, sem.at[1]),
    ]
    for copy in copies:
        copy.start()
    for copy in copies:
        copy.wait()


def per_device(field_bricks, owners, bricks, corners, fraction):
    devices = lax.axis_size("map")
    trajectories_here, quarter = owners.shape
    row_count = trajectories_here * quarter
    capacity = 4 * row_count // devices
    tiles = 2 * -(-capacity // (2 * LANES))
    chunks = row_count // LANES
    lines = 4 * tiles
    buffer = jax.ShapeDtypeStruct((devices, lines + 8, LANES), jnp.float32)
    flat = jax.ShapeDtypeStruct((chunks, LANES), jnp.int32)
    vm = pl.BlockSpec(memory_space=VMEM)
    sm = pl.BlockSpec(memory_space=SMEM)
    hbm = pl.BlockSpec(memory_space=pltpu.HBM)
    whole = VMEM((quarter, trajectories_here), jnp.int32)
    outgoing, own, rank, meta, field = pl.pallas_call(
        functools.partial(dispatch_kernel, devices, tiles),
        out_shape=(buffer, flat, flat, flat, jax.ShapeDtypeStruct(field_bricks.shape, field_bricks.dtype)),
        in_specs=[hbm] * 5,
        out_specs=(vm,) * 5,
        scratch_shapes=[
            VMEM((chunks, 8, LANES), jnp.float32),
            VMEM((chunks, LANES), jnp.int32),
            SMEM((chunks, LANES), jnp.int32),
            pltpu.SemaphoreType.DMA(()),
            whole, whole, whole,
            VMEM((3, quarter, trajectories_here), jnp.float32),
            pltpu.SemaphoreType.DMA((5,)),
        ]
        + [VMEM((lines + 8, LANES), jnp.float32)] * (devices if devices <= 8 else 0),
        compiler_params=pltpu.CompilerParams(vmem_limit_bytes=16 << 20),
        name="dispatch",
    )(*(stay(x) for x in (owners.T, bricks.T, corners.T, fraction.transpose(0, 2, 1), field_bricks)))
    sems = pltpu.SemaphoreType.DMA((devices,))
    reps = lax.axis_size("rep")
    rep_sems = pltpu.SemaphoreType.DMA((reps,))
    batch = batch_of(tiles)
    square = VMEM((2 if batch % 2 == 0 else 1, 2, LANES, LANES), jnp.float32)
    bricks = field_bricks.shape[0]
    cost, waypoint_grad = pl.pallas_call(
        functools.partial(fused_kernel, devices, reps, tiles),
        out_shape=(
            jax.ShapeDtypeStruct((1, trajectories_here), jnp.float32),
            jax.ShapeDtypeStruct((3, quarter, trajectories_here), jnp.float32),
        ),
        in_specs=[vm] * 5,
        out_specs=(vm, vm),
        scratch_shapes=[
            SMEM((chunks, LANES), jnp.int32),
            VMEM((bricks * 7, LANES), jnp.float32),
            VMEM((devices * lines, LANES), jnp.float32),
            VMEM((devices * lines, LANES), jnp.float32),
            VMEM((devices - 2, lines + 8, LANES), jnp.float32),
            VMEM((2, lines + 8, LANES), jnp.float32),
            VMEM((2, 2 * batch, LANES), jnp.int32),
            SMEM((2, 2 * batch, LANES), jnp.int32),
            square,
            VMEM((chunks, 8, LANES), jnp.float32),
            VMEM((reps, 1, trajectories_here), jnp.float32),
            pltpu.SemaphoreType.DMA(()),
            pltpu.SemaphoreType.DMA((2,)),
            sems, sems, sems, sems, rep_sems, rep_sems,
        ],
        compiler_params=pltpu.CompilerParams(collective_id=0, has_side_effects=True, vmem_limit_bytes=24 << 20),
        name="fused",
    )(outgoing, field, own, rank, meta)
    cost, waypoint_grad = pl.pallas_call(
        finish_kernel,
        out_shape=(
            jax.ShapeDtypeStruct(cost.shape, jnp.float32),
            jax.ShapeDtypeStruct(waypoint_grad.shape, jnp.float32),
        ),
        in_specs=[vm] * 2,
        out_specs=(hbm,) * 2,
        scratch_shapes=[pltpu.SemaphoreType.DMA((2,))],
        compiler_params=pltpu.CompilerParams(vmem_limit_bytes=1 << 20),
        name="finish",
    )(cost, waypoint_grad)
    return cost.reshape(trajectories_here), waypoint_grad.transpose(0, 2, 1)


def solution(mesh):
    placed = (
        P("map", None),
        P("map", "rep"),
        P("map", "rep"),
        P("map", "rep"),
        P(None, "map", "rep"),
    )
    return jax.shard_map(
        per_device,
        mesh=mesh,
        in_specs=placed,
        out_specs=(P("map"), P(None, "map", "rep")),
        check_vma=False,
    )
```
